32 devices in a mesh: seq: 4 (over z), tp: 4 (over y, x), dp: 2 (over core).
Axes of the slice: x: 2, y: 2, z: 4, core: 2. Of those that a mesh axis runs over, the one named last changes fastest.
Arguments:
- x_ckpt: bfloat16 [1024, 5120], P(('dp', 'seq', 'tp')), parts along dimension 0, may hold values from -5 to 5
- bc_ckpt: bfloat16 [2, 1024, 128], P(None, ('dp', 'seq', 'tp')), parts along dimension 1, may hold values from -1 to 1
- step_sizes: float32 [80, 1024], P('tp', ('dp', 'seq')), parts along dimension 1, may hold values from 0.03 to 0.3
- decay_rate: float32 [80], P('tp'), may hold values from 0 to 1, as said below
- skip_gain: float32 [80], P('tp'), may hold values from 0.25 to 1.75
- grad_out: bfloat16 [1024, 5120], P(('dp', 'seq'), 'tp'), parts along dimension 0, may hold values from -3 to 3
Outputs:
- grad_x: bfloat16 [1024, 5120], P(('dp', 'seq'), 'tp'), parts along dimension 0
- grad_bc: float32 [2, 1024, 128], P(None, ('dp', 'seq', 'tp')), parts along dimension 1
- grad_step: float32 [80, 1024], P('tp', ('dp', 'seq')), parts along dimension 1
The draws below stay inside these ranges and needn't reach their ends.
There are 2 independent parts, one for each index of `dp`. The reference program is written for one: setup_inputs(seed, part) draws one part's arguments, and reference() takes and returns one part's arrays. A program takes and returns all parts, laid end to end along the dimension named above; an argument that names none is the same for every part. Nothing has to cross between parts.
Inputs may be any that keep to these rules, and one draw needn't show every extreme that they name: `decay_rate`: positive decay rates of the 80 heads.
All inputs are finite; a program needn't handle non-finite values.
Results may differ from the reference program's by a relative error of at most 0.001.
Values may be sent and summed in bfloat16 or wider, within the bound.
No kernel may reach another device: no remote copies, remote signals or barrier semaphores. Data moves between devices by JAX's collectives and lax.ppermute only.
A program may use at most 128 MiB of HBM per device.

```python
import math
from functools import partial
import jax
import jax.numpy as jnp
from jax import lax

HEADS = 80
STATE = 128
BLOCK = 128
TOKENS = 512
INNER = 5120


def draw_decay_rate(key, part):
    rate_key = jax.random.fold_in(key, 11)
    top_rate = 0.5
    low_rate = 20.0 / TOKENS
    drawn = jax.random.uniform(rate_key, (HEADS,), minval=math.log(low_rate), maxval=math.log(top_rate))
    return jnp.exp(drawn).astype(jnp.float32)


def draw_step_sizes(key, part):
    level_key, factor_key = jax.random.split(jax.random.fold_in(key, 23))
    level = jnp.exp(jax.random.uniform(level_key, (HEADS, 1), minval=math.log(0.043), maxval=math.log(0.187)))
    factor = jnp.exp(jax.random.uniform(factor_key, (HEADS, TOKENS), minval=math.log(0.7), maxval=math.log(1.6)))
    return jnp.clip(level * factor, 0.03, 0.3).astype(jnp.float32)


def draw_bc_ckpt(key, part):
    sign_key, noise_key = jax.random.split(jax.random.fold_in(key, 37))
    direction = jnp.where(jax.random.bernoulli(sign_key, 0.5, (STATE,)), 1.0, -1.0)
    common = direction / (8.0 * math.sqrt(STATE))
    spread = 1.0 / math.sqrt(STATE)
    noise = jnp.clip(jax.random.normal(noise_key, (2, TOKENS, STATE)), -4.0, 4.0) * spread
    return jnp.clip(common[None, None, :] + noise, -1.0, 1.0).astype(jnp.bfloat16)


def draw_x_ckpt(key, part):
    offset_key, noise_key = jax.random.split(jax.random.fold_in(key, 41))
    offset = jnp.clip(0.8 * jax.random.normal(offset_key, (1, INNER)), -2.5, 2.5)
    noise = jnp.clip(0.6 * jax.random.normal(noise_key, (TOKENS, INNER)), -2.4, 2.4)
    return jnp.clip(offset + noise, -5.0, 5.0).astype(jnp.bfloat16)


def draw_grad_out(key, part):
    offset_key, noise_key = jax.random.split(jax.random.fold_in(key, 53))
    offset = jnp.clip(0.4 * jax.random.normal(offset_key, (1, INNER)), -1.5, 1.5)
    noise = jnp.clip(0.4 * jax.random.normal(noise_key, (TOKENS, INNER)), -1.5, 1.5)
    return jnp.clip(offset + noise, -3.0, 3.0).astype(jnp.bfloat16)


def setup_inputs(seed: int = 0, part: int = 0) -> dict:
    key_of = jax.random.split(jax.random.key(seed), 7)
    part_splits = jax.random.split(jax.random.fold_in(key_of[6], part), 7)
    return {
        "x_ckpt": draw_x_ckpt(jax.random.fold_in(jax.random.fold_in(key_of[6], part), 71), part),
        "bc_ckpt": draw_bc_ckpt(jax.random.fold_in(jax.random.fold_in(key_of[6], part), 71), part),
        "step_sizes": draw_step_sizes(jax.random.fold_in(jax.random.fold_in(key_of[6], part), 71), part),
        "decay_rate": draw_decay_rate(jax.random.fold_in(key_of[6], 71), part),
        "skip_gain": jnp.clip(1.0 + 0.15 * jax.random.normal(key_of[4], (HEADS,), jnp.float32), 0.25, 1.75),
        "grad_out": draw_grad_out(jax.random.fold_in(jax.random.fold_in(key_of[6], part), 71), part),
    }


highest = lax.Precision.HIGHEST

def block_step(head_rates, head_gains, carry_state, pieces):
    inputs, step_block, proj_b, proj_c = pieces
    head_count = step_block.shape[0]
    row_count = step_block.shape[1]
    values = inputs.astype(jnp.float32).reshape(row_count, head_count, -1)
    cumulative = jnp.cumsum(-head_rates[:, None] * step_block, axis=1)
    positions = jnp.arange(row_count, dtype=jnp.int32)
    causal = positions[:, None] >= positions[None, :]
    log_gaps = cumulative[:, :, None] - cumulative[:, None, :]
    within = jnp.where(causal, jnp.exp(jnp.where(causal, log_gaps, 0.0)), 0.0)
    scores = jnp.dot(proj_c, proj_b.T, precision=highest, preferred_element_type=jnp.float32)
    weights = within * scores[None, :, :] * step_block[:, None, :]
    local_part = jnp.einsum('hts,shp->thp', weights, values, precision=highest, preferred_element_type=jnp.float32)
    carried = jnp.einsum('tn,hpn->thp', proj_c, carry_state, precision=highest, preferred_element_type=jnp.float32)
    carried = carried * jnp.exp(cumulative).T[:, :, None]
    result = local_part + carried + head_gains[None, :, None] * values
    tail_weight = jnp.exp(cumulative[:, -1:] - cumulative) * step_block
    fresh_state = jnp.einsum('hs,shp,sn->hpn', tail_weight, values, proj_b, precision=highest, preferred_element_type=jnp.float32)
    final_state = jnp.exp(cumulative[:, -1])[:, None, None] * carry_state + fresh_state
    return (final_state, result.reshape(row_count, -1))

def run_blocks(inputs, step_sizes, proj_b, proj_c, start_state, head_rates, head_gains, block_rows):
    row_count = inputs.shape[0]
    block_count = row_count // block_rows
    head_count = step_sizes.shape[0]
    input_blocks = inputs.reshape(block_count, block_rows, inputs.shape[1])
    step_blocks = step_sizes.reshape(head_count, block_count, block_rows).transpose(1, 0, 2)
    b_blocks = proj_b.reshape(block_count, block_rows, proj_b.shape[1])
    c_blocks = proj_c.reshape(block_count, block_rows, proj_c.shape[1])
    stepper = jax.checkpoint(partial(block_step, head_rates, head_gains))
    final_state, results = lax.scan(stepper, start_state, (input_blocks, step_blocks, b_blocks, c_blocks))
    return (results.reshape(row_count, -1), final_state)

def reference(x_ckpt, bc_ckpt, step_sizes, decay_rate, skip_gain, grad_out):
    head_count = decay_rate.shape[0]
    head_width = x_ckpt.shape[1] // head_count
    proj_b = bc_ckpt[0].astype(jnp.float32)
    proj_c = bc_ckpt[1].astype(jnp.float32)
    start_state = jnp.zeros((head_count, head_width, proj_b.shape[1]), jnp.float32)

    def forward(inputs, basis_b, basis_c, step_block):
        output, final_state = run_blocks(inputs, step_block, basis_b, basis_c, start_state, decay_rate, skip_gain, BLOCK)
        return output
    output, pull_back = jax.vjp(forward, x_ckpt, proj_b, proj_c, step_sizes)
    grad_x, grad_b, grad_c, grad_step = pull_back(grad_out.astype(jnp.float32))
    return (grad_x, jnp.stack([grad_b, grad_c]), grad_step)
```

```python
from functools import partial

import jax
import jax.numpy as jnp
import numpy as np
from jax import lax
from jax.experimental import pallas as pl
from jax.experimental.pallas import tpu as pltpu
from jax.sharding import Mesh, PartitionSpec as P

F32 = jnp.float32
BF16 = jnp.bfloat16
LANES = 128
NEVER = -1e30


def dot(a, b, dims=((1,), (0,))):
    return lax.dot_general(a, b, (dims, ((), ())), preferred_element_type=F32)


def two(a):
    high = a.astype(BF16)
    return high, (a - high.astype(F32)).astype(BF16)


def three(a):
    high = a.astype(BF16)
    rest = a - high.astype(F32)
    mid = rest.astype(BF16)
    return high, mid, (rest - mid.astype(F32)).astype(BF16)


def dots(parts, b, dims=((1,), (0,))):
    total = dot(parts[0], b, dims)
    for part in parts[1:]:
        total = total + dot(part, b, dims)
    return total


def below(rows, cols, test):
    i = lax.broadcasted_iota(jnp.int32, (rows, cols), 0)
    j = lax.broadcasted_iota(jnp.int32, (rows, cols), 1)
    return jnp.where(test(i, j), 1.0, 0.0).astype(BF16)


def lead(heads):
    return -(-heads // 16) * 16


class Sizes:
    def __init__(self, heads, rows, columns, state):
        self.heads = heads // 2
        self.rows = rows
        self.tokens = 2 * rows
        self.width = columns // 2
        self.head_width = self.width // self.heads
        self.state = state
        self.lead = lead(self.heads)

    def spread(self):
        return below(self.lead, self.width, lambda i, j: j // self.head_width == i)


def by_head(z, parts):
    spread = z.spread()
    total = dot(spread, parts[0], ((1,), (1,)))
    for part in parts[1:]:
        total = total + dot(spread, part, ((1,), (1,)))
    return total


def tables(z, place, step, message, rates):
    first = place[1] == 0
    own = jnp.where(first, step[: z.heads, :], step[z.heads :, :])
    if z.lead > z.heads:
        own = jnp.concatenate([own, jnp.ones((z.lead - z.heads, z.rows), F32)], axis=0)
    tail = message[z.rows : z.rows + z.lead, : 3 * z.rows].astype(F32)
    other = tail[:, : z.rows] + tail[:, z.rows : 2 * z.rows] + tail[:, 2 * z.rows : 3 * z.rows]
    steps = jnp.concatenate([jnp.where(first, own, other), jnp.where(first, other, own)], axis=1)
    logs = steps * (-rates[:, :1])
    upto = below(z.tokens, z.tokens, lambda i, j: i <= j)
    return steps, dots(three(logs), upto)


def gradient(z, place, grad, message):
    first = place[1] == 0
    own = jnp.where(first, grad[:, : z.width], grad[:, z.width :])
    other = message[: z.rows, :]
    return jnp.concatenate([jnp.where(first, own, other), jnp.where(first, other, own)], axis=0)


def weighted(z, forward, steps, sums, values, upstream):
    tail = steps * jnp.exp(sums[:, -1:] - sums)
    scale = dots(three(jnp.where(forward, tail, jnp.exp(sums))), z.spread(), ((0,), (0,)))
    source = jnp.where(forward, values, upstream).astype(F32)
    return scale, scale * source


def first_kernel(z, modes, place, step, message, rates, grad, packed, state, dy, table):
    steps, sums = tables(z, place, step, message, rates)
    upstream = gradient(z, place, grad, message)
    dy[...] = upstream
    table[: z.lead, :] = steps
    table[z.lead : 2 * z.lead, :] = sums
    values = packed[:, : z.width]
    for k in range(modes):
        forward = place[2 + k] == 0
        scale, rows = weighted(z, forward, steps, sums, values, upstream)
        basis = jnp.where(
            forward,
            packed[:, z.width : z.width + z.state],
            packed[:, z.width + z.state :],
        )
        high, low = two(rows)
        found = dot(basis, high, ((0,), (0,))) + dot(basis, low, ((0,), (0,)))
        if modes == 1:
            top = jnp.max(jnp.abs(found), axis=0, keepdims=True)
            power = jnp.ceil(jnp.log2(jnp.maximum(top, 1e-30)))
            state[k, : z.state, :] = found * jnp.exp2(-power)
            state[k, z.state :, :] = jnp.broadcast_to(power, (8, z.width))
        else:
            passing = jnp.broadcast_to(jnp.exp(sums[:, -1:]), (z.lead, LANES))
            state[k, : z.state, :] = found
            state[k, z.state :, :] = dots(three(passing), z.spread(), ((0,), (0,)))[:8, :]


def local_kernel(z, packed, dy, table, gains, dx, gb, sums_out, mixed):
    n, half = z.tokens, z.rows
    steps = table[: z.lead, :]
    sums = table[z.lead : 2 * z.lead, :]
    source = jnp.log(steps) - sums
    pad = jnp.zeros((LANES - z.lead, n), F32)
    columns = jnp.transpose(jnp.concatenate([source, pad], axis=0))
    b = packed[:, z.width : z.width + z.state]
    c = packed[:, z.width + z.state :]
    scores = dot(b, c, ((1,), (1,)))
    mixed[...] = jnp.zeros((n, n), F32)
    per = LANES // z.head_width
    lane = lax.broadcasted_iota(jnp.int32, (n, LANES), 1) // z.head_width
    read = []
    for block in range(z.width // LANES):
        at = slice(block * LANES, (block + 1) * LANES)
        values = packed[:, at]
        upstream = dy[:, at]
        total = jnp.zeros((n, LANES), F32)
        for k in range(per):
            h = block * per + k
            own = jnp.where(lane == k, upstream, jnp.zeros_like(upstream))
            row = sums[h : h + 1, :]
            pieces = []
            drawn = jnp.zeros((1, n), F32)
            for part in range(2):
                s = slice(part * half, (part + 1) * half)
                t = slice(part * half, n)
                wide = n - part * half
                i = lax.broadcasted_iota(jnp.int32, (half, wide), 0)
                j = lax.broadcasted_iota(jnp.int32, (half, wide), 1)
                gap = row[:, t] + columns[s, h : h + 1]
                decay = jnp.exp(jnp.where(j >= i, gap, NEVER))
                pairs = decay * dot(values[s, :], own[t, :], ((1,), (1,)))
                mixed[s, t] += pairs
                score = scores[s, t]
                seen = jnp.sum(pairs * score, axis=0, keepdims=True)
                if part:
                    seen = jnp.concatenate([jnp.zeros((1, half), F32), seen], axis=1)
                drawn = drawn + seen
                high, low = two(decay * score)
                pieces.append(dot(high, own[t, :]) + dot(low, own[t, :]))
            read.append(drawn)
            total = total + jnp.concatenate(pieces, axis=0)
        dx[:, at] = total
    seen = jnp.concatenate(read + [jnp.zeros((z.lead - z.heads, n), F32)], axis=0)
    given = by_head(z, two(packed[:, : z.width].astype(F32) * dx[...]))
    sums_out[: z.lead, :] = seen - given
    sums_out[z.lead : 2 * z.lead, :] = given
    dx[...] = dx[...] + gains[:1, :] * dy[...].astype(F32)
    high, low = two(mixed[...])
    gb[0] = dot(high, c) + dot(low, c)
    gb[1] = dot(high, b, ((0,), (0,))) + dot(low, b, ((0,), (0,)))


def last_kernel(z, modes, place, packed, dy, table, dx, gb, sums_in, rates, state, out, own, partner, grad_step):
    n = z.tokens
    steps = table[: z.lead, :]
    sums = table[z.lead : 2 * z.lead, :]
    later = sums_in[: z.lead, :]
    given = sums_in[z.lead : 2 * z.lead, :]
    earlier = jnp.zeros_like(later)
    total = dx[...]
    extra = [gb[0], gb[1]]
    values = packed[:, : z.width]
    upstream = dy[...]
    whole = []
    for k in range(modes):
        forward = place[2 + k] == 0
        scale, rows = weighted(z, forward, steps, sums, values, upstream)
        basis = jnp.where(
            forward,
            packed[:, z.width : z.width + z.state],
            packed[:, z.width + z.state :],
        )
        came = state[k, : z.state, :] * jnp.exp2(state[k, z.state : z.state + 1, :])
        whole.append(came)
        high, low = two(came)
        carried = dot(basis, high) + dot(basis, low)
        rows_high, rows_low = two(rows)
        grown = (
            dot(rows_high, high, ((1,), (1,)))
            + dot(rows_high, low, ((1,), (1,)))
            + dot(rows_low, high, ((1,), (1,)))
        )
        none = jnp.zeros_like(grown)
        extra = [extra[0] + jnp.where(forward, grown, none), extra[1] + jnp.where(forward, none, grown)]
        found = by_head(z, two(rows * carried))
        empty = jnp.zeros_like(found)
        later = later + jnp.where(forward, empty, found)
        earlier = earlier + jnp.where(forward, found, empty)
        given = given + jnp.where(forward, found, empty)
        total = total + jnp.where(forward, scale * carried, jnp.zeros_like(scale))
    decays = dots(three(later), below(n, n, lambda i, j: i >= j)) + dots(
        three(earlier), below(n, n, lambda i, j: i < j)
    )
    if modes == 2:
        both = by_head(z, three(whole[0] * whole[1]))
        both = jnp.sum(both, axis=1, keepdims=True) * jnp.exp(sums[:, -1:])
        decays = decays + both
    steps_grad = given / steps - rates[:, :1] * decays
    first = place[1] == 0
    half = z.rows
    early, late = total[:half, :].astype(BF16), total[half:, :].astype(BF16)
    own[...] = jnp.where(first, early, late)
    partner[:half, :] = jnp.where(first, late, early)
    early, late = steps_grad[:, :half], steps_grad[:, half:]
    grad_step[...] = jnp.where(first, early, late)
    partner[half:, :] = jnp.zeros((z.lead, z.width), BF16)
    high, low = two(jnp.where(first, late, early))
    partner[half:, :half] = high
    partner[half:, half : 2 * half] = low
    chunk = out.shape[2]
    for k in range(out.shape[0]):
        out[k, 0] = extra[0][k * chunk : (k + 1) * chunk, :]
        out[k, 1] = extra[1][k * chunk : (k + 1) * chunk, :]


def call(kernel, out_shape, scalars, arrays, flops, scratch=()):
    vmem = pl.BlockSpec(memory_space=pltpu.VMEM)
    smem = pl.BlockSpec(memory_space=pltpu.SMEM)
    return pl.pallas_call(
        kernel,
        out_shape=out_shape,
        in_specs=[smem] * len(scalars) + [vmem] * len(arrays),
        out_specs=jax.tree.map(lambda _: vmem, out_shape),
        scratch_shapes=scratch,
        compiler_params=pltpu.CompilerParams(vmem_limit_bytes=40 * 1024 * 1024),
        cost_estimate=pl.CostEstimate(flops=flops, bytes_accessed=2_000_000, transcendentals=0),
    )(*scalars, *arrays)


def keep(a):
    return lax.reduce_precision(a, 8, 7)


def chain(state, passing, size, index, reverse):
    ring = [(i, i + 1) for i in range(size - 1)]
    if reverse:
        ring = [(j, i) for i, j in ring]
    place = size - 1 - index if reverse else index

    def hop(k, carry):
        entering, leaving = carry
        came = lax.ppermute(leaving, "pair", ring)
        here = place == k
        return (
            jnp.where(here, came, entering),
            jnp.where(here, passing * came + state, leaving),
        )

    return lax.fori_loop(1, size, hop, (jnp.zeros_like(state), state))[0]


def shards(x_ckpt, bc_ckpt, step_sizes, decay_rate, skip_gain, grad_out):
    heads, rows = step_sizes.shape
    z = Sizes(heads, rows, grad_out.shape[1], bc_ckpt.shape[2])
    pairs, tp = lax.axis_size("pair"), lax.axis_size("tp")
    pair, member = lax.axis_index("pair"), lax.axis_index("member")
    swap = [(0, 1), (1, 0)]
    other = 1 - member
    modes = 1 if pairs == 2 else 2
    kinds = [pair] if modes == 1 else [jnp.int32(0), jnp.int32(1)]
    place = jnp.stack([pair, member, *kinds]).astype(jnp.int32)

    sent = lax.dynamic_slice(grad_out, (0, other * z.width), (rows, z.width))
    step = lax.dynamic_slice(step_sizes, (other * z.heads, 0), (z.heads, rows))
    high = keep(step)
    mid = keep(step - high)
    low = step - high - mid
    tail = jnp.concatenate([high, mid, low], axis=1).astype(BF16)
    tail = jnp.pad(
        tail,
        ((0, z.lead - z.heads), (0, z.width - 3 * rows)),
        constant_values=np.asarray(1.0, BF16),
    )
    message = lax.ppermute(jnp.concatenate([sent, tail], axis=0), "member", swap)

    tokens = x_ckpt.shape[0]
    slots = x_ckpt.reshape(tokens, tp, 2, z.width).transpose(2, 1, 0, 3).reshape(2 * tp, tokens, z.width)
    shared = bc_ckpt.transpose(1, 0, 2).reshape(1, tokens, 2 * z.state)
    slots = jnp.concatenate([slots, jnp.broadcast_to(shared, (2 * tp, tokens, 2 * z.state))], axis=2)
    packed = lax.all_to_all(slots, ("member", "tp"), split_axis=0, concat_axis=0, tiled=True)
    packed = packed.reshape(z.tokens, z.width + 2 * z.state)

    mine = lax.dynamic_slice(decay_rate, (member * z.heads,), (z.heads,))
    rates = jnp.broadcast_to(jnp.pad(mine, (0, z.lead - z.heads))[:, None], (z.lead, LANES))
    mine = lax.dynamic_slice(skip_gain, (member * z.heads,), (z.heads,))
    gains = jnp.broadcast_to(jnp.repeat(mine, z.head_width)[None, :], (8, z.width))

    shape = jax.ShapeDtypeStruct
    state, dy, table = call(
        partial(first_kernel, z, modes),
        [
            shape((modes, z.state + 8, z.width), F32),
            shape((z.tokens, z.width), BF16),
            shape((2 * z.lead, z.tokens), F32),
        ],
        [place],
        [step_sizes, message, rates, grad_out, packed],
        4 * z.tokens * z.state * z.width,
    )
    if modes == 1:
        turn = lax.ppermute(state.astype(jnp.float16), "pair", swap)
        came = turn.astype(F32)
    else:
        passing = state[0, z.state :, :][:1]
        forth = chain(state[0, : z.state], passing, pairs, pair, False)
        back = chain(state[1, : z.state], passing, pairs, pair, True)
        came = jnp.pad(jnp.stack([back, forth]), ((0, 0), (0, 8), (0, 0)))

    dx, gb, sums = call(
        partial(local_kernel, z),
        [
            shape((z.tokens, z.width), F32),
            shape((2, z.tokens, z.state), F32),
            shape((2 * z.lead, z.tokens), F32),
        ],
        [],
        [packed, dy, table, gains],
        12 * z.tokens * z.tokens * z.width,
        [pltpu.VMEM((z.tokens, z.tokens), F32)],
    )
    out, own, partner, grad_step = call(
        partial(last_kernel, z, modes),
        [
            shape((2 * tp, 2, tokens, z.state), F32),
            shape((rows, z.width), BF16),
            shape((rows + z.lead, z.width), BF16),
            shape((z.lead, rows), F32),
        ],
        [place],
        [packed, dy, table, dx, gb, sums, rates, came],
        12 * z.tokens * z.state * z.width,
    )
    swapped = lax.ppermute(partner, "member", swap)
    gathered = lax.all_to_all(out, ("member", "tp"), split_axis=0, concat_axis=0, tiled=True)
    grad_bc = jnp.sum(gathered, axis=0)
    first = member == 0
    theirs = swapped[:rows]
    grad_x = jnp.where(
        first,
        jnp.concatenate([own, theirs], axis=1),
        jnp.concatenate([theirs, own], axis=1),
    )
    tail = swapped[rows : rows + z.heads].astype(F32)
    theirs = tail[:, :rows] + tail[:, rows : 2 * rows]
    mine = grad_step[: z.heads]
    grad_step = jnp.where(
        first,
        jnp.concatenate([mine, theirs], axis=0),
        jnp.concatenate([theirs, mine], axis=0),
    )
    return (grad_x, grad_bc, grad_step)


def solution(mesh):
    sizes = dict(mesh.shape)
    names = []
    for name in mesh.axis_names:
        names += ["pair", "member"] if name == "seq" else [name]
    shape = []
    for name in mesh.axis_names:
        shape += [sizes[name] // 2, 2] if name == "seq" else [sizes[name]]
    fine = Mesh(mesh.devices.reshape(shape), tuple(names))
    seq = ("dp", "pair", "member")
    return jax.shard_map(
        shards,
        mesh=fine,
        in_specs=(
            P((*seq, "tp"), None),
            P(None, (*seq, "tp"), None),
            P("tp", seq),
            P("tp"),
            P("tp"),
            P(seq, "tp"),
        ),
        out_specs=(
            P(seq, "tp"),
            P(None, (*seq, "tp"), None),
            P("tp", seq),
        ),
        check_vma=False,
    )
```

```python
from functools import partial

import jax
import jax.numpy as jnp
from jax import lax
from jax.experimental import pallas as pl
from jax.experimental.pallas import tpu as pltpu
from jax.sharding import Mesh, PartitionSpec as P

F32 = jnp.float32
BF16 = jnp.bfloat16
LANES = 128
NEVER = -1e30


def dot(a, b, dims=((1,), (0,))):
    return lax.dot_general(a, b, (dims, ((), ())), preferred_element_type=F32)


def two(a):
    high = a.astype(BF16)
    return high, (a - high.astype(F32)).astype(BF16)


def three(a):
    high = a.astype(BF16)
    rest = a - high.astype(F32)
    mid = rest.astype(BF16)
    return high, mid, (rest - mid.astype(F32)).astype(BF16)


def dots(parts, b, dims=((1,), (0,))):
    total = dot(parts[0], b, dims)
    for part in parts[1:]:
        total = total + dot(part, b, dims)
    return total


def below(rows, cols, test):
    i = lax.broadcasted_iota(jnp.int32, (rows, cols), 0)
    j = lax.broadcasted_iota(jnp.int32, (rows, cols), 1)
    return jnp.where(test(i, j), 1.0, 0.0).astype(BF16)


def lead(heads):
    return -(-heads // 16) * 16


class Sizes:
    def __init__(self, heads, rows, columns, state):
        self.heads = heads // 2
        self.rows = rows
        self.tokens = 2 * rows
        self.width = columns // 2
        self.head_width = self.width // self.heads
        self.state = state
        self.lead = lead(self.heads)

    def spread(self):
        return below(self.lead, self.width, lambda i, j: j // self.head_width == i)


def by_head(z, parts):
    spread = z.spread()
    total = dot(spread, parts[0], ((1,), (1,)))
    for part in parts[1:]:
        total = total + dot(spread, part, ((1,), (1,)))
    return total


def tables(z, place, step, message, rates):
    first = place[1] == 0
    own = jnp.where(first, step[: z.heads, :], step[z.heads :, :])
    if z.lead > z.heads:
        own = jnp.concatenate([own, jnp.ones((z.lead - z.heads, z.rows), F32)], axis=0)
    tail = message[z.rows : z.rows + z.lead, : 3 * z.rows].astype(F32)
    other = tail[:, : z.rows] + tail[:, z.rows : 2 * z.rows] + tail[:, 2 * z.rows : 3 * z.rows]
    steps = jnp.concatenate([jnp.where(first, own, other), jnp.where(first, other, own)], axis=1)
    logs = steps * (-rates[:, :1])
    upto = below(z.tokens, z.tokens, lambda i, j: i <= j)
    return steps, dots(three(logs), upto)


def gradient(z, place, grad, message):
    first = place[1] == 0
    own = jnp.where(first, grad[:, : z.width], grad[:, z.width :])
    other = message[: z.rows, :]
    return jnp.concatenate([jnp.where(first, own, other), jnp.where(first, other, own)], axis=0)


def send_kernel(z, place, grad, step, message):
    first = place[1] == 0
    message[: z.rows, :] = jnp.where(first, grad[:, z.width :], grad[:, : z.width])
    steps = jnp.where(first, step[z.heads :, :], step[: z.heads, :])
    if z.lead > z.heads:
        steps = jnp.concatenate([steps, jnp.ones((z.lead - z.heads, z.rows), F32)], axis=0)
    message[z.rows :, :] = jnp.zeros((z.lead, z.width), BF16)
    for k, part in enumerate(three(steps)):
        message[z.rows :, k * z.rows : (k + 1) * z.rows] = part


def pack_kernel(z, x, bc, slots):
    count = slots.shape[0] // 2
    for member in range(2):
        for k in range(count):
            at = (2 * k + member) * z.width
            slots[member * count + k, :, : z.width] = x[:, at : at + z.width]
            slots[member * count + k, :, z.width : z.width + z.state] = bc[0]
            slots[member * count + k, :, z.width + z.state :] = bc[1]


def prepare_kernel(z, modes, place, step, message, rates, grad, dy, table, scales):
    steps, sums = tables(z, place, step, message, rates)
    dy[...] = gradient(z, place, grad, message)
    table[: z.lead, :] = steps
    table[z.lead : 2 * z.lead, :] = sums
    tail = steps * jnp.exp(sums[:, -1:] - sums)
    for k in range(modes):
        chosen = jnp.where(place[2 + k] == 0, tail, jnp.exp(sums))
        scales[k] = dots(three(chosen), z.spread(), ((0,), (0,)))


def weighted(z, forward, scale, packed, dy):
    source = jnp.where(forward, packed[:, : z.width], dy[...]).astype(F32)
    basis = jnp.where(
        forward,
        packed[:, z.width : z.width + z.state],
        packed[:, z.width + z.state :],
    )
    return scale * source, basis


def state_kernel(z, modes, place, packed, dy, table, scales, state):
    for k in range(modes):
        rows, basis = weighted(z, place[2 + k] == 0, scales[k], packed, dy)
        high, low = two(rows)
        found = dot(basis, high, ((0,), (0,))) + dot(basis, low, ((0,), (0,)))
        if modes == 1:
            top = jnp.max(jnp.abs(found), axis=0, keepdims=True)
            power = jnp.ceil(jnp.log2(jnp.maximum(top, 1e-30)))
            state[k, : z.state, :] = found * jnp.exp2(-power)
            state[k, z.state :, :] = jnp.broadcast_to(power, (8, z.width))
        else:
            sums = table[z.lead : 2 * z.lead, :]
            passing = jnp.broadcast_to(jnp.exp(sums[:, -1:]), (z.lead, LANES))
            state[k, : z.state, :] = found
            state[k, z.state :, :] = dots(three(passing), z.spread(), ((0,), (0,)))[:8, :]


def local_kernel(z, packed, dy, table, gains, dx, gb, sums_out, mixed):
    n, half = z.tokens, z.rows
    steps = table[: z.lead, :]
    sums = table[z.lead : 2 * z.lead, :]
    source = jnp.log(steps) - sums
    pad = jnp.zeros((LANES - z.lead, n), F32)
    columns = jnp.transpose(jnp.concatenate([source, pad], axis=0))
    b = packed[:, z.width : z.width + z.state]
    c = packed[:, z.width + z.state :]
    scores = dot(b, c, ((1,), (1,)))
    mixed[...] = jnp.zeros((n, n), F32)
    per = LANES // z.head_width
    lane = lax.broadcasted_iota(jnp.int32, (n, LANES), 1) // z.head_width
    read = []
    for block in range(z.width // LANES):
        at = slice(block * LANES, (block + 1) * LANES)
        values = packed[:, at]
        upstream = dy[:, at]
        total = jnp.zeros((n, LANES), F32)
        for k in range(per):
            h = block * per + k
            own = jnp.where(lane == k, upstream, jnp.zeros_like(upstream))
            row = sums[h : h + 1, :]
            pieces = []
            drawn = jnp.zeros((1, n), F32)
            for part in range(2):
                s = slice(part * half, (part + 1) * half)
                t = slice(part * half, n)
                wide = n - part * half
                i = lax.broadcasted_iota(jnp.int32, (half, wide), 0)
                j = lax.broadcasted_iota(jnp.int32, (half, wide), 1)
                gap = row[:, t] + columns[s, h : h + 1]
                decay = jnp.exp(jnp.where(j >= i, gap, NEVER))
                pairs = decay * dot(values[s, :], own[t, :], ((1,), (1,)))
                mixed[s, t] += pairs
                score = scores[s, t]
                seen = jnp.sum(pairs * score, axis=0, keepdims=True)
                if part:
                    seen = jnp.concatenate([jnp.zeros((1, half), F32), seen], axis=1)
                drawn = drawn + seen
                high, low = two(decay * score)
                pieces.append(dot(high, own[t, :]) + dot(low, own[t, :]))
            read.append(drawn)
            total = total + jnp.concatenate(pieces, axis=0)
        dx[:, at] = total
    seen = jnp.concatenate(read + [jnp.zeros((z.lead - z.heads, n), F32)], axis=0)
    given = by_head(z, two(packed[:, : z.width].astype(F32) * dx[...]))
    sums_out[: z.lead, :] = seen - given
    sums_out[z.lead : 2 * z.lead, :] = given
    dx[...] = dx[...] + gains[:1, :] * dy[...].astype(F32)
    high, low = two(mixed[...])
    gb[0] = dot(high, c) + dot(low, c)
    gb[1] = dot(high, b, ((0,), (0,))) + dot(low, b, ((0,), (0,)))


def last_kernel(z, modes, place, packed, dy, table, scales, dx, gb, sums_in, rates, state, out, own, partner, grad_step):
    n = z.tokens
    steps = table[: z.lead, :]
    sums = table[z.lead : 2 * z.lead, :]
    later = sums_in[: z.lead, :]
    given = sums_in[z.lead : 2 * z.lead, :]
    earlier = jnp.zeros_like(later)
    total = dx[...]
    extra = [gb[0], gb[1]]
    whole = []
    for k in range(modes):
        forward = place[2 + k] == 0
        scale = scales[k]
        rows, basis = weighted(z, forward, scale, packed, dy)
        came = state[k, : z.state, :] * jnp.exp2(state[k, z.state : z.state + 1, :])
        whole.append(came)
        high, low = two(came)
        carried = dot(basis, high) + dot(basis, low)
        rows_high, rows_low = two(rows)
        grown = (
            dot(rows_high, high, ((1,), (1,)))
            + dot(rows_high, low, ((1,), (1,)))
            + dot(rows_low, high, ((1,), (1,)))
        )
        none = jnp.zeros_like(grown)
        extra = [extra[0] + jnp.where(forward, grown, none), extra[1] + jnp.where(forward, none, grown)]
        found = by_head(z, two(rows * carried))
        empty = jnp.zeros_like(found)
        later = later + jnp.where(forward, empty, found)
        earlier = earlier + jnp.where(forward, found, empty)
        given = given + jnp.where(forward, found, empty)
        total = total + jnp.where(forward, scale * carried, jnp.zeros_like(scale))
    decays = dots(three(later), below(n, n, lambda i, j: i >= j)) + dots(
        three(earlier), below(n, n, lambda i, j: i < j)
    )
    if modes == 2:
        both = by_head(z, three(whole[0] * whole[1]))
        both = jnp.sum(both, axis=1, keepdims=True) * jnp.exp(sums[:, -1:])
        decays = decays + both
    steps_grad = given / steps - rates[:, :1] * decays
    first = place[1] == 0
    half = z.rows
    early, late = total[:half, :].astype(BF16), total[half:, :].astype(BF16)
    own[...] = jnp.where(first, early, late)
    partner[:half, :] = jnp.where(first, late, early)
    early, late = steps_grad[:, :half], steps_grad[:, half:]
    grad_step[...] = jnp.where(first, early, late)
    partner[half:, :] = jnp.zeros((z.lead, z.width), BF16)
    high, low = two(jnp.where(first, late, early))
    partner[half:, :half] = high
    partner[half:, half : 2 * half] = low
    chunk = out.shape[2]
    for k in range(out.shape[0]):
        out[k, 0] = extra[0][k * chunk : (k + 1) * chunk, :]
        out[k, 1] = extra[1][k * chunk : (k + 1) * chunk, :]


def call(kernel, out_shape, scalars, arrays, flops, scratch=()):
    vmem = pl.BlockSpec(memory_space=pltpu.VMEM)
    smem = pl.BlockSpec(memory_space=pltpu.SMEM)
    return pl.pallas_call(
        kernel,
        out_shape=out_shape,
        in_specs=[smem] * len(scalars) + [vmem] * len(arrays),
        out_specs=jax.tree.map(lambda _: vmem, out_shape),
        scratch_shapes=scratch,
        compiler_params=pltpu.CompilerParams(vmem_limit_bytes=40 * 1024 * 1024),
        cost_estimate=pl.CostEstimate(flops=flops, bytes_accessed=2_000_000, transcendentals=0),
    )(*scalars, *arrays)


def chain(state, passing, size, index, reverse):
    ring = [(i, i + 1) for i in range(size - 1)]
    if reverse:
        ring = [(j, i) for i, j in ring]
    place = size - 1 - index if reverse else index

    def hop(k, carry):
        entering, leaving = carry
        came = lax.ppermute(leaving, "pair", ring)
        here = place == k
        return (
            jnp.where(here, came, entering),
            jnp.where(here, passing * came + state, leaving),
        )

    return lax.fori_loop(1, size, hop, (jnp.zeros_like(state), state))[0]


def shards(x_ckpt, bc_ckpt, step_sizes, decay_rate, skip_gain, grad_out):
    heads, rows = step_sizes.shape
    z = Sizes(heads, rows, grad_out.shape[1], bc_ckpt.shape[2])
    pairs, tp = lax.axis_size("pair"), lax.axis_size("tp")
    pair, member = lax.axis_index("pair"), lax.axis_index("member")
    swap = [(0, 1), (1, 0)]
    modes = 1 if pairs == 2 else 2
    kinds = [pair] if modes == 1 else [jnp.int32(0), jnp.int32(1)]
    place = jnp.stack([pair, member, *kinds]).astype(jnp.int32)

    shape = jax.ShapeDtypeStruct
    tokens = x_ckpt.shape[0]
    (message,) = call(
        partial(send_kernel, z),
        [shape((rows + z.lead, z.width), BF16)],
        [place],
        [grad_out, step_sizes],
        1000,
    )
    message = lax.ppermute(message, "member", swap)
    (slots,) = call(
        partial(pack_kernel, z),
        [shape((2 * tp, tokens, z.width + 2 * z.state), BF16)],
        [],
        [x_ckpt, bc_ckpt],
        1000,
    )
    packed = lax.all_to_all(slots, ("member", "tp"), split_axis=0, concat_axis=0, tiled=True)
    packed = packed.reshape(z.tokens, z.width + 2 * z.state)

    mine = lax.dynamic_slice(decay_rate, (member * z.heads,), (z.heads,))
    rates = jnp.broadcast_to(jnp.pad(mine, (0, z.lead - z.heads))[:, None], (z.lead, LANES))
    mine = lax.dynamic_slice(skip_gain, (member * z.heads,), (z.heads,))
    gains = jnp.broadcast_to(jnp.repeat(mine, z.head_width)[None, :], (8, z.width))

    dy, table, scales = call(
        partial(prepare_kernel, z, modes),
        [
            shape((z.tokens, z.width), BF16),
            shape((2 * z.lead, z.tokens), F32),
            shape((modes, z.tokens, z.width), F32),
        ],
        [place],
        [step_sizes, message, rates, grad_out],
        1_000_000,
    )
    (state,) = call(
        partial(state_kernel, z, modes),
        [shape((modes, z.state + 8, z.width), F32)],
        [place],
        [packed, dy, table, scales],
        4 * z.tokens * z.state * z.width,
    )
    if modes == 1:
        turn = lax.ppermute(state.astype(jnp.float16), "pair", swap)
        came = turn.astype(F32)
    else:
        passing = state[0, z.state :, :][:1]
        forth = chain(state[0, : z.state], passing, pairs, pair, False)
        back = chain(state[1, : z.state], passing, pairs, pair, True)
        came = jnp.pad(jnp.stack([back, forth]), ((0, 0), (0, 8), (0, 0)))

    dx, gb, sums = call(
        partial(local_kernel, z),
        [
            shape((z.tokens, z.width), F32),
            shape((2, z.tokens, z.state), F32),
            shape((2 * z.lead, z.tokens), F32),
        ],
        [],
        [packed, dy, table, gains],
        12 * z.tokens * z.tokens * z.width,
        [pltpu.VMEM((z.tokens, z.tokens), F32)],
    )
    out, own, partner, grad_step = call(
        partial(last_kernel, z, modes),
        [
            shape((2 * tp, 2, tokens, z.state), F32),
            shape((rows, z.width), BF16),
            shape((rows + z.lead, z.width), BF16),
            shape((z.lead, rows), F32),
        ],
        [place],
        [packed, dy, table, scales, dx, gb, sums, rates, came],
        12 * z.tokens * z.state * z.width,
    )
    swapped = lax.ppermute(partner, "member", swap)
    gathered = lax.all_to_all(out, ("member", "tp"), split_axis=0, concat_axis=0, tiled=True)
    grad_bc = jnp.sum(gathered, axis=0)
    first = member == 0
    theirs = swapped[:rows]
    grad_x = jnp.where(
        first,
        jnp.concatenate([own, theirs], axis=1),
        jnp.concatenate([theirs, own], axis=1),
    )
    tail = swapped[rows : rows + z.heads].astype(F32)
    theirs = tail[:, :rows] + tail[:, rows : 2 * rows]
    mine = grad_step[: z.heads]
    grad_step = jnp.where(
        first,
        jnp.concatenate([mine, theirs], axis=0),
        jnp.concatenate([theirs, mine], axis=0),
    )
    return (grad_x, grad_bc, grad_step)


def solution(mesh):
    sizes = dict(mesh.shape)
    names = []
    for name in mesh.axis_names:
        names += ["pair", "member"] if name == "seq" else [name]
    shape = []
    for name in mesh.axis_names:
        shape += [sizes[name] // 2, 2] if name == "seq" else [sizes[name]]
    fine = Mesh(mesh.devices.reshape(shape), tuple(names))
    seq = ("dp", "pair", "member")
    return jax.shard_map(
        shards,
        mesh=fine,
        in_specs=(
            P((*seq, "tp"), None),
            P(None, (*seq, "tp"), None),
            P("tp", seq),
            P("tp"),
            P("tp"),
            P(seq, "tp"),
        ),
        out_specs=(
            P(seq, "tp"),
            P(None, (*seq, "tp"), None),
            P("tp", seq),
        ),
        check_vma=False,
    )
```

```python
from functools import partial

import jax
import jax.numpy as jnp
from jax import lax
from jax.experimental import pallas as pl
from jax.experimental.pallas import tpu as pltpu
from jax.sharding import Mesh, PartitionSpec as P

F32 = jnp.float32
BF16 = jnp.bfloat16
LANES = 128
NEVER = -1e30


def dot(a, b, dims=((1,), (0,))):
    return lax.dot_general(a, b, (dims, ((), ())), preferred_element_type=F32)


def two(a):
    high = a.astype(BF16)
    return high, (a - high.astype(F32)).astype(BF16)


def three(a):
    high = a.astype(BF16)
    rest = a - high.astype(F32)
    mid = rest.astype(BF16)
    return high, mid, (rest - mid.astype(F32)).astype(BF16)


def dots(parts, b, dims=((1,), (0,))):
    total = dot(parts[0], b, dims)
    for part in parts[1:]:
        total = total + dot(part, b, dims)
    return total


def below(rows, cols, test):
    i = lax.broadcasted_iota(jnp.int32, (rows, cols), 0)
    j = lax.broadcasted_iota(jnp.int32, (rows, cols), 1)
    return jnp.where(test(i, j), 1.0, 0.0).astype(BF16)


def lead(heads):
    return -(-heads // 16) * 16


class Sizes:
    def __init__(self, heads, rows, columns, state):
        self.heads = heads // 2
        self.rows = rows
        self.tokens = 2 * rows
        self.width = columns // 2
        self.head_width = self.width // self.heads
        self.state = state
        self.lead = lead(self.heads)

    def spread(self):
        return below(self.lead, self.width, lambda i, j: j // self.head_width == i)


def by_head(z, parts):
    spread = z.spread()
    total = dot(spread, parts[0], ((1,), (1,)))
    for part in parts[1:]:
        total = total + dot(spread, part, ((1,), (1,)))
    return total


def tables(z, place, step, message, rates):
    first = place[1] == 0
    own = jnp.where(first, step[: z.heads, :], step[z.heads :, :])
    if z.lead > z.heads:
        own = jnp.concatenate([own, jnp.ones((z.lead - z.heads, z.rows), F32)], axis=0)
    tail = message[z.rows : z.rows + z.lead, : 3 * z.rows].astype(F32)
    other = tail[:, : z.rows] + tail[:, z.rows : 2 * z.rows] + tail[:, 2 * z.rows : 3 * z.rows]
    steps = jnp.concatenate([jnp.where(first, own, other), jnp.where(first, other, own)], axis=1)
    logs = steps * (-rates[:, :1])
    upto = below(z.tokens, z.tokens, lambda i, j: i <= j)
    return steps, dots(three(logs), upto)


def gradient(z, place, grad, message):
    first = place[1] == 0
    own = jnp.where(first, grad[:, : z.width], grad[:, z.width :])
    other = message[: z.rows, :]
    return jnp.concatenate([jnp.where(first, own, other), jnp.where(first, other, own)], axis=0)


def send_kernel(z, place, grad, step, message, held, sems):
    first = place[1] == 0
    at = pl.multiple_of((1 - place[1]) * z.width, LANES)
    sizes = pltpu.make_async_copy(step, held, sems.at[0])
    rows = pltpu.make_async_copy(grad.at[:, pl.ds(at, z.width)], message.at[pl.ds(0, z.rows), :], sems.at[1])
    rows.start()
    sizes.start()
    message[z.rows :, :] = jnp.zeros((z.lead, z.width), BF16)
    sizes.wait()
    steps = jnp.where(first, held[z.heads :, :], held[: z.heads, :])
    if z.lead > z.heads:
        steps = jnp.concatenate([steps, jnp.ones((z.lead - z.heads, z.rows), F32)], axis=0)
    for k, part in enumerate(three(steps)):
        message[z.rows :, k * z.rows : (k + 1) * z.rows] = part
    rows.wait()


def pack_kernel(z, x, bc, slots):
    count = slots.shape[0] // 2
    for member in range(2):
        for k in range(count):
            at = (2 * k + member) * z.width
            slots[member * count + k, :, : z.width] = x[:, at : at + z.width]
            slots[member * count + k, :, z.width : z.width + z.state] = bc[0]
            slots[member * count + k, :, z.width + z.state :] = bc[1]


def prepare_kernel(z, modes, place, step, message, rates, grad, dy, table, scales):
    steps, sums = tables(z, place, step, message, rates)
    dy[...] = gradient(z, place, grad, message)
    table[: z.lead, :] = steps
    table[z.lead : 2 * z.lead, :] = sums
    tail = steps * jnp.exp(sums[:, -1:] - sums)
    for k in range(modes):
        chosen = jnp.where(place[2 + k] == 0, tail, jnp.exp(sums))
        scales[k] = dots(three(chosen), z.spread(), ((0,), (0,)))


def weighted(z, forward, scale, packed, dy):
    source = jnp.where(forward, packed[:, : z.width], dy[...]).astype(F32)
    basis = jnp.where(
        forward,
        packed[:, z.width : z.width + z.state],
        packed[:, z.width + z.state :],
    )
    return scale * source, basis


def state_kernel(z, modes, place, packed, dy, table, scales, state):
    for k in range(modes):
        rows, basis = weighted(z, place[2 + k] == 0, scales[k], packed, dy)
        high, low = two(rows)
        found = dot(basis, high, ((0,), (0,))) + dot(basis, low, ((0,), (0,)))
        if modes == 1:
            top = jnp.max(jnp.abs(found), axis=0, keepdims=True)
            power = jnp.ceil(jnp.log2(jnp.maximum(top, 1e-30)))
            state[k, : z.state, :] = found * jnp.exp2(-power)
            state[k, z.state :, :] = jnp.broadcast_to(power, (8, z.width))
        else:
            sums = table[z.lead : 2 * z.lead, :]
            passing = jnp.broadcast_to(jnp.exp(sums[:, -1:]), (z.lead, LANES))
            state[k, : z.state, :] = found
            state[k, z.state :, :] = dots(three(passing), z.spread(), ((0,), (0,)))[:8, :]


def local_kernel(z, modes, place, packed, dy, table, scales, rates, gains, dx, gb, base, scaled, mixed):
    n, half = z.tokens, z.rows
    steps = table[: z.lead, :]
    sums = table[z.lead : 2 * z.lead, :]
    source = jnp.log(steps) - sums
    pad = jnp.zeros((LANES - z.lead, n), F32)
    columns = jnp.transpose(jnp.concatenate([source, pad], axis=0))
    b = packed[:, z.width : z.width + z.state]
    c = packed[:, z.width + z.state :]
    scores = dot(b, c, ((1,), (1,)))
    mixed[...] = jnp.zeros((n, n), F32)
    per = LANES // z.head_width
    lane = lax.broadcasted_iota(jnp.int32, (n, LANES), 1) // z.head_width
    read = []
    for block in range(z.width // LANES):
        at = slice(block * LANES, (block + 1) * LANES)
        values = packed[:, at]
        upstream = dy[:, at]
        total = jnp.zeros((n, LANES), F32)
        for k in range(per):
            h = block * per + k
            own = jnp.where(lane == k, upstream, jnp.zeros_like(upstream))
            row = sums[h : h + 1, :]
            pieces = []
            drawn = jnp.zeros((1, n), F32)
            for part in range(2):
                s = slice(part * half, (part + 1) * half)
                t = slice(part * half, n)
                wide = n - part * half
                i = lax.broadcasted_iota(jnp.int32, (half, wide), 0)
                j = lax.broadcasted_iota(jnp.int32, (half, wide), 1)
                gap = row[:, t] + columns[s, h : h + 1]
                decay = jnp.exp(jnp.where(j >= i, gap, NEVER))
                pairs = decay * dot(values[s, :], own[t, :], ((1,), (1,)))
                mixed[s, t] += pairs
                score = scores[s, t]
                seen = jnp.sum(pairs * score, axis=0, keepdims=True)
                if part:
                    seen = jnp.concatenate([jnp.zeros((1, half), F32), seen], axis=1)
                drawn = drawn + seen
                high, low = two(decay * score)
                pieces.append(dot(high, own[t, :]) + dot(low, own[t, :]))
            read.append(drawn)
            total = total + jnp.concatenate(pieces, axis=0)
        dx[:, at] = total
    seen = jnp.concatenate(read + [jnp.zeros((z.lead - z.heads, n), F32)], axis=0)
    given = by_head(z, two(packed[:, : z.width].astype(F32) * dx[...]))
    later = below(n, n, lambda i, j: i >= j)
    base[...] = given / steps - rates[:, :1] * dots(three(seen - given), later)
    dx[...] = dx[...] + gains[:1, :] * dy[...].astype(F32)
    high, low = two(mixed[...])
    gb[0] = dot(high, c) + dot(low, c)
    gb[1] = dot(high, b, ((0,), (0,))) + dot(low, b, ((0,), (0,)))
    for k in range(modes):
        rows, _ = weighted(z, place[2 + k] == 0, scales[k], packed, dy)
        high, low = two(rows)
        scaled[2 * k] = high
        scaled[2 * k + 1] = low


def arrived(z, state, k):
    return state[k, : z.state, :] * jnp.exp2(state[k, z.state : z.state + 1, :])


def share_kernel(z, modes, place, gb, scaled, state, out):
    extra = [gb[0], gb[1]]
    for k in range(modes):
        high, low = two(arrived(z, state, k))
        grown = (
            dot(scaled[2 * k], high, ((1,), (1,)))
            + dot(scaled[2 * k], low, ((1,), (1,)))
            + dot(scaled[2 * k + 1], high, ((1,), (1,)))
        )
        none = jnp.zeros_like(grown)
        forward = place[2 + k] == 0
        extra = [extra[0] + jnp.where(forward, grown, none), extra[1] + jnp.where(forward, none, grown)]
    chunk = out.shape[2]
    for k in range(out.shape[0]):
        out[k, 0] = extra[0][k * chunk : (k + 1) * chunk, :]
        out[k, 1] = extra[1][k * chunk : (k + 1) * chunk, :]


def rest_kernel(z, modes, place, packed, table, scales, scaled, dx, base, rates, state, own, partner, grad_step):
    n = z.tokens
    steps = table[: z.lead, :]
    total = dx[...]
    decays = jnp.zeros_like(steps)
    steps_grad = base[...]
    states = []
    for k in range(modes):
        forward = place[2 + k] == 0
        basis = jnp.where(
            forward,
            packed[:, z.width : z.width + z.state],
            packed[:, z.width + z.state :],
        )
        came = arrived(z, state, k)
        states.append(came)
        high, low = two(came)
        carried = dot(basis, high) + dot(basis, low)
        total = total + jnp.where(forward, scales[k], jnp.zeros_like(carried)) * carried
        rows = scaled[2 * k].astype(F32) + scaled[2 * k + 1].astype(F32)
        found = by_head(z, two(rows * carried))
        i = lax.broadcasted_iota(jnp.int32, (n, n), 0)
        j = lax.broadcasted_iota(jnp.int32, (n, n), 1)
        reach = (j - i) * jnp.where(forward, 1, -1) >= jnp.where(forward, 1, 0)
        decays = decays + dots(three(found), jnp.where(reach, 1.0, 0.0).astype(BF16))
        steps_grad = steps_grad + jnp.where(forward, found, jnp.zeros_like(found)) / steps
    if modes == 2:
        sums = table[z.lead : 2 * z.lead, :]
        both = by_head(z, three(states[0] * states[1]))
        decays = decays + jnp.sum(both, axis=1, keepdims=True) * jnp.exp(sums[:, -1:])
    steps_grad = steps_grad - rates[:, :1] * decays
    first = place[1] == 0
    half = z.rows
    early, late = total[:half, :].astype(BF16), total[half:, :].astype(BF16)
    own[...] = jnp.where(first, early, late)
    partner[:half, :] = jnp.where(first, late, early)
    early, late = steps_grad[:, :half], steps_grad[:, half:]
    grad_step[...] = jnp.where(first, early, late)
    partner[half:, :] = jnp.zeros((z.lead, z.width), BF16)
    high, low = two(jnp.where(first, late, early))
    partner[half:, :half] = high
    partner[half:, half : 2 * half] = low


def call(kernel, out_shape, scalars, arrays, flops, scratch=(), space=pltpu.VMEM):
    vmem = pl.BlockSpec(memory_space=pltpu.VMEM)
    given = pl.BlockSpec(memory_space=space)
    smem = pl.BlockSpec(memory_space=pltpu.SMEM)
    return pl.pallas_call(
        kernel,
        out_shape=out_shape,
        in_specs=[smem] * len(scalars) + [given] * len(arrays),
        out_specs=jax.tree.map(lambda _: vmem, out_shape),
        scratch_shapes=scratch,
        compiler_params=pltpu.CompilerParams(vmem_limit_bytes=40 * 1024 * 1024),
        cost_estimate=pl.CostEstimate(flops=flops, bytes_accessed=2_000_000, transcendentals=0),
    )(*scalars, *arrays)


def chain(state, passing, size, index, reverse):
    ring = [(i, i + 1) for i in range(size - 1)]
    if reverse:
        ring = [(j, i) for i, j in ring]
    place = size - 1 - index if reverse else index

    def hop(k, carry):
        entering, leaving = carry
        came = lax.ppermute(leaving, "pair", ring)
        here = place == k
        return (
            jnp.where(here, came, entering),
            jnp.where(here, passing * came + state, leaving),
        )

    return lax.fori_loop(1, size, hop, (jnp.zeros_like(state), state))[0]


def shards(x_ckpt, bc_ckpt, step_sizes, decay_rate, skip_gain, grad_out):
    heads, rows = step_sizes.shape
    z = Sizes(heads, rows, grad_out.shape[1], bc_ckpt.shape[2])
    pairs, tp = lax.axis_size("pair"), lax.axis_size("tp")
    pair, member = lax.axis_index("pair"), lax.axis_index("member")
    swap = [(0, 1), (1, 0)]
    modes = 1 if pairs == 2 else 2
    kinds = [pair] if modes == 1 else [jnp.int32(0), jnp.int32(1)]
    place = jnp.stack([pair, member, *kinds]).astype(jnp.int32)

    shape = jax.ShapeDtypeStruct
    tokens = x_ckpt.shape[0]
    (message,) = call(
        partial(send_kernel, z),
        [shape((rows + z.lead, z.width), BF16)],
        [place],
        [grad_out, step_sizes],
        1000,
        [pltpu.VMEM((heads, rows), F32), pltpu.SemaphoreType.DMA((2,))],
        pltpu.HBM,
    )
    message = lax.ppermute(message, "member", swap)
    (slots,) = call(
        partial(pack_kernel, z),
        [shape((2 * tp, tokens, z.width + 2 * z.state), BF16)],
        [],
        [x_ckpt, bc_ckpt],
        1000,
    )
    packed = lax.all_to_all(slots, ("member", "tp"), split_axis=0, concat_axis=0, tiled=True)
    packed = packed.reshape(z.tokens, z.width + 2 * z.state)

    mine = lax.dynamic_slice(decay_rate, (member * z.heads,), (z.heads,))
    rates = jnp.broadcast_to(jnp.pad(mine, (0, z.lead - z.heads))[:, None], (z.lead, LANES))
    mine = lax.dynamic_slice(skip_gain, (member * z.heads,), (z.heads,))
    gains = jnp.broadcast_to(jnp.repeat(mine, z.head_width)[None, :], (8, z.width))

    dy, table, scales = call(
        partial(prepare_kernel, z, modes),
        [
            shape((z.tokens, z.width), BF16),
            shape((2 * z.lead, z.tokens), F32),
            shape((modes, z.tokens, z.width), F32),
        ],
        [place],
        [step_sizes, message, rates, grad_out],
        1_000_000,
    )
    (state,) = call(
        partial(state_kernel, z, modes),
        [shape((modes, z.state + 8, z.width), F32)],
        [place],
        [packed, dy, table, scales],
        4 * z.tokens * z.state * z.width,
    )
    if modes == 1:
        turn = lax.ppermute(state.astype(jnp.float16), "pair", swap)
        came = turn.astype(F32)
    else:
        passing = state[0, z.state :, :][:1]
        forth = chain(state[0, : z.state], passing, pairs, pair, False)
        back = chain(state[1, : z.state], passing, pairs, pair, True)
        came = jnp.pad(jnp.stack([back, forth]), ((0, 0), (0, 8), (0, 0)))

    dx, gb, base, scaled = call(
        partial(local_kernel, z, modes),
        [
            shape((z.tokens, z.width), F32),
            shape((2, z.tokens, z.state), F32),
            shape((z.lead, z.tokens), F32),
            shape((2 * modes, z.tokens, z.width), BF16),
        ],
        [place],
        [packed, dy, table, scales, rates, gains],
        12 * z.tokens * z.tokens * z.width,
        [pltpu.VMEM((z.tokens, z.tokens), F32)],
    )
    (out,) = call(
        partial(share_kernel, z, modes),
        [shape((2 * tp, 2, tokens, z.state), F32)],
        [place],
        [gb, scaled, came],
        6 * z.tokens * z.state * z.width,
    )
    gathered = lax.all_to_all(out, ("member", "tp"), split_axis=0, concat_axis=0, tiled=True)
    own, partner, grad_step = call(
        partial(rest_kernel, z, modes),
        [
            shape((rows, z.width), BF16),
            shape((rows + z.lead, z.width), BF16),
            shape((z.lead, rows), F32),
        ],
        [place],
        [packed, table, scales, scaled, dx, base, rates, came],
        12 * z.tokens * z.state * z.width,
    )
    swapped = lax.ppermute(partner, "member", swap)
    grad_bc = jnp.sum(gathered, axis=0)
    first = member == 0
    theirs = swapped[:rows]
    grad_x = jnp.where(
        first,
        jnp.concatenate([own, theirs], axis=1),
        jnp.concatenate([theirs, own], axis=1),
    )
    tail = swapped[rows : rows + z.heads].astype(F32)
    theirs = tail[:, :rows] + tail[:, rows : 2 * rows]
    mine = grad_step[: z.heads]
    grad_step = jnp.where(
        first,
        jnp.concatenate([mine, theirs], axis=0),
        jnp.concatenate([theirs, mine], axis=0),
    )
    return (grad_x, grad_bc, grad_step)


def solution(mesh):
    sizes = dict(mesh.shape)
    names = []
    for name in mesh.axis_names:
        names += ["pair", "member"] if name == "seq" else [name]
    shape = []
    for name in mesh.axis_names:
        shape += [sizes[name] // 2, 2] if name == "seq" else [sizes[name]]
    fine = Mesh(mesh.devices.reshape(shape), tuple(names))
    seq = ("dp", "pair", "member")
    return jax.shard_map(
        shards,
        mesh=fine,
        in_specs=(
            P((*seq, "tp"), None),
            P(None, (*seq, "tp"), None),
            P("tp", seq),
            P("tp"),
            P("tp"),
            P(seq, "tp"),
        ),
        out_specs=(
            P(seq, "tp"),
            P(None, (*seq, "tp"), None),
            P("tp", seq),
        ),
        check_vma=False,
    )
```

```python
from functools import partial

import jax
import jax.numpy as jnp
from jax import lax
from jax.experimental import pallas as pl
from jax.experimental.pallas import tpu as pltpu
from jax.sharding import Mesh, PartitionSpec as P

F32 = jnp.float32
BF16 = jnp.bfloat16
LANES = 128
NEVER = -1e30
OPENING_VMEM = 66_800_000


def dot(a, b, dims=((1,), (0,))):
    return lax.dot_general(a, b, (dims, ((), ())), preferred_element_type=F32)


def two(a):
    high = a.astype(BF16)
    return high, (a - high.astype(F32)).astype(BF16)


def three(a):
    high = a.astype(BF16)
    rest = a - high.astype(F32)
    mid = rest.astype(BF16)
    return high, mid, (rest - mid.astype(F32)).astype(BF16)


def dots(parts, b, dims=((1,), (0,))):
    total = dot(parts[0], b, dims)
    for part in parts[1:]:
        total = total + dot(part, b, dims)
    return total


def below(rows, cols, test):
    i = lax.broadcasted_iota(jnp.int32, (rows, cols), 0)
    j = lax.broadcasted_iota(jnp.int32, (rows, cols), 1)
    return jnp.where(test(i, j), 1.0, 0.0).astype(BF16)


def lead(heads):
    return -(-heads // 16) * 16


class Sizes:
    def __init__(self, heads, rows, columns, state):
        self.heads = heads // 2
        self.rows = rows
        self.tokens = 2 * rows
        self.width = columns // 2
        self.head_width = self.width // self.heads
        self.state = state
        self.lead = lead(self.heads)
        self.blocks = self.width // LANES
        self.state_rows = self.blocks * state + -(-self.blocks // 8) * 8

    def spread(self):
        return below(self.lead, self.width, lambda i, j: j // self.head_width == i)


def exponent(a):
    top = jnp.max(jnp.abs(a), axis=0, keepdims=True)
    return jnp.ceil(jnp.log2(jnp.maximum(top, 1e-30)))


def by_head(z, parts):
    spread = z.spread()
    total = dot(spread, parts[0], ((1,), (1,)))
    for part in parts[1:]:
        total = total + dot(spread, part, ((1,), (1,)))
    return total


def tables(z, place, step, message, rates):
    first = place[1] == 0
    own = jnp.where(first, step[: z.heads, :], step[z.heads :, :])
    if z.lead > z.heads:
        own = jnp.concatenate([own, jnp.ones((z.lead - z.heads, z.rows), F32)], axis=0)
    tail = message[z.rows : z.rows + z.lead, : 3 * z.rows].astype(F32)
    other = tail[:, : z.rows] + tail[:, z.rows : 2 * z.rows] + tail[:, 2 * z.rows : 3 * z.rows]
    steps = jnp.concatenate([jnp.where(first, own, other), jnp.where(first, other, own)], axis=1)
    logs = steps * (-rates[:, :1])
    upto = below(z.tokens, z.tokens, lambda i, j: i <= j)
    return steps, dots(three(logs), upto)


def gradient(z, place, grad, message):
    first = place[1] == 0
    own = jnp.where(first, grad[:, : z.width], grad[:, z.width :])
    other = message[: z.rows, :]
    return jnp.concatenate([jnp.where(first, own, other), jnp.where(first, other, own)], axis=0)


def open_kernel(z, grad, step, x, bc, message, slots, held, shared, stage, note, sems):
    index = lax.axis_index("member")
    first = index == 0
    count = slots.shape[0]
    at = pl.multiple_of((1 - index) * z.width, LANES)
    sizes = pltpu.make_async_copy(step, held, sems.at[0])
    basis = pltpu.make_async_copy(bc, shared, sems.at[1])
    rows = pltpu.make_async_copy(grad.at[:, pl.ds(at, z.width)], note.at[pl.ds(0, z.rows), :], sems.at[2])
    sent = pltpu.make_async_copy(note, message, sems.at[3 + 2 * count])
    taken, given = [], []
    for k in range(count):
        member, peer = divmod(k, count // 2)
        columns = pl.ds((2 * peer + member) * z.width, z.width)
        taken.append(
            pltpu.make_async_copy(x.at[:, columns], stage.at[k, :, pl.ds(0, z.width)], sems.at[3 + k])
        )
        given.append(pltpu.make_async_copy(stage.at[k], slots.at[k], sems.at[3 + count + k]))
    for copy in (sizes, rows, basis, *taken):
        copy.start()
    note[z.rows :, :] = jnp.zeros((z.lead, z.width), BF16)
    sizes.wait()
    steps = jnp.where(first, held[z.heads :, :], held[: z.heads, :])
    if z.lead > z.heads:
        steps = jnp.concatenate([steps, jnp.ones((z.lead - z.heads, z.rows), F32)], axis=0)
    for k, part in enumerate(three(steps)):
        note[z.rows :, k * z.rows : (k + 1) * z.rows] = part
    rows.wait()
    sent.start()
    basis.wait()
    for k in range(count):
        stage[k, :, z.width : z.width + z.state] = shared[0]
        stage[k, :, z.width + z.state :] = shared[1]
    for k in range(count):
        taken[k].wait()
        given[k].start()
    for copy in (sent, *given):
        copy.wait()


def prepare_kernel(z, modes, place, step, message, rates, grad, dy, table, scales):
    steps, sums = tables(z, place, step, message, rates)
    dy[...] = gradient(z, place, grad, message)
    table[: z.lead, :] = steps
    table[z.lead : 2 * z.lead, :] = sums
    tail = steps * jnp.exp(sums[:, -1:] - sums)
    for k in range(modes):
        chosen = jnp.where(place[2 + k] == 0, tail, jnp.exp(sums))
        scales[k] = dots(three(chosen), z.spread(), ((0,), (0,)))


def weighted(z, forward, scale, packed, dy):
    source = jnp.where(forward, packed[:, : z.width], dy[...]).astype(F32)
    basis = jnp.where(
        forward,
        packed[:, z.width : z.width + z.state],
        packed[:, z.width + z.state :],
    )
    return scale * source, basis


def state_kernel(z, modes, place, packed, dy, table, scales, state):
    for k in range(modes):
        rows, basis = weighted(z, place[2 + k] == 0, scales[k], packed, dy)
        high, low = two(rows)
        found = dot(basis, high, ((0,), (0,))) + dot(basis, low, ((0,), (0,)))
        if modes == 1:
            power = exponent(found)
            found = found * jnp.exp2(-power)
        else:
            sums = table[z.lead : 2 * z.lead, :]
            passing = jnp.broadcast_to(jnp.exp(sums[:, -1:]), (z.lead, LANES))
            power = dots(three(passing), z.spread(), ((0,), (0,)))[:1, :]
        for block in range(z.blocks):
            at = slice(block * LANES, (block + 1) * LANES)
            state[k, block * z.state : (block + 1) * z.state, :] = found[:, at]
            state[k, z.blocks * z.state + block : z.blocks * z.state + block + 1, :] = power[:, at]
        left = state.shape[1] - z.blocks * (z.state + 1)
        if left:
            state[k, z.blocks * (z.state + 1) :, :] = jnp.zeros((left, LANES), F32)


def local_kernel(z, modes, place, packed, dy, table, scales, rates, gains, dx, gb, base, scaled, mixed):
    n, half = z.tokens, z.rows
    steps = table[: z.lead, :]
    sums = table[z.lead : 2 * z.lead, :]
    source = jnp.log(steps) - sums
    pad = jnp.zeros((LANES - z.lead, n), F32)
    columns = jnp.transpose(jnp.concatenate([source, pad], axis=0))
    b = packed[:, z.width : z.width + z.state]
    c = packed[:, z.width + z.state :]
    scores = dot(b, c, ((1,), (1,)))
    mixed[...] = jnp.zeros((n, n), F32)
    per = LANES // z.head_width
    lane = lax.broadcasted_iota(jnp.int32, (n, LANES), 1) // z.head_width
    read = []
    for block in range(z.width // LANES):
        at = slice(block * LANES, (block + 1) * LANES)
        values = packed[:, at]
        upstream = dy[:, at]
        total = jnp.zeros((n, LANES), F32)
        for k in range(per):
            h = block * per + k
            own = jnp.where(lane == k, upstream, jnp.zeros_like(upstream))
            row = sums[h : h + 1, :]
            pieces = []
            drawn = jnp.zeros((1, n), F32)
            for part in range(2):
                s = slice(part * half, (part + 1) * half)
                t = slice(part * half, n)
                wide = n - part * half
                i = lax.broadcasted_iota(jnp.int32, (half, wide), 0)
                j = lax.broadcasted_iota(jnp.int32, (half, wide), 1)
                gap = row[:, t] + columns[s, h : h + 1]
                decay = jnp.exp(jnp.where(j >= i, gap, NEVER))
                pairs = decay * dot(values[s, :], own[t, :], ((1,), (1,)))
                mixed[s, t] += pairs
                score = scores[s, t]
                seen = jnp.sum(pairs * score, axis=0, keepdims=True)
                if part:
                    seen = jnp.concatenate([jnp.zeros((1, half), F32), seen], axis=1)
                drawn = drawn + seen
                high, low = two(decay * score)
                pieces.append(dot(high, own[t, :]) + dot(low, own[t, :]))
            read.append(drawn)
            total = total + jnp.concatenate(pieces, axis=0)
        dx[:, at] = total
    seen = jnp.concatenate(read + [jnp.zeros((z.lead - z.heads, n), F32)], axis=0)
    given = by_head(z, two(packed[:, : z.width].astype(F32) * dx[...]))
    later = below(n, n, lambda i, j: i >= j)
    base[...] = given / steps - rates[:, :1] * dots(three(seen - given), later)
    dx[...] = dx[...] + gains[:1, :] * dy[...].astype(F32)
    high, low = two(mixed[...])
    gb[0] = dot(high, c) + dot(low, c)
    gb[1] = dot(high, b, ((0,), (0,))) + dot(low, b, ((0,), (0,)))
    for k in range(modes):
        rows, _ = weighted(z, place[2 + k] == 0, scales[k], packed, dy)
        high, low = two(rows)
        scaled[2 * k] = high
        scaled[2 * k + 1] = low


def arrived(z, state, k):
    parts = []
    for block in range(z.blocks):
        power = state[k, z.blocks * z.state + block : z.blocks * z.state + block + 1, :]
        parts.append(state[k, block * z.state : (block + 1) * z.state, :] * jnp.exp2(power))
    return jnp.concatenate(parts, axis=1)


def last_kernel(z, modes, place, packed, table, scales, scaled, dx, base, gb, rates, state, out, own, partner, grad_step):
    n = z.tokens
    steps = table[: z.lead, :]
    total = dx[...]
    extra = [gb[0], gb[1]]
    decays = jnp.zeros_like(steps)
    steps_grad = base[...]
    states = []
    for k in range(modes):
        forward = place[2 + k] == 0
        basis = jnp.where(
            forward,
            packed[:, z.width : z.width + z.state],
            packed[:, z.width + z.state :],
        )
        came = arrived(z, state, k)
        states.append(came)
        high, low = two(came)
        carried = dot(basis, high) + dot(basis, low)
        total = total + jnp.where(forward, scales[k], jnp.zeros_like(carried)) * carried
        rows = scaled[2 * k].astype(F32) + scaled[2 * k + 1].astype(F32)
        found = by_head(z, two(rows * carried))
        i = lax.broadcasted_iota(jnp.int32, (n, n), 0)
        j = lax.broadcasted_iota(jnp.int32, (n, n), 1)
        reach = (j - i) * jnp.where(forward, 1, -1) >= jnp.where(forward, 1, 0)
        decays = decays + dots(three(found), jnp.where(reach, 1.0, 0.0).astype(BF16))
        steps_grad = steps_grad + jnp.where(forward, found, jnp.zeros_like(found)) / steps
        grown = (
            dot(scaled[2 * k], high, ((1,), (1,)))
            + dot(scaled[2 * k], low, ((1,), (1,)))
            + dot(scaled[2 * k + 1], high, ((1,), (1,)))
        )
        none = jnp.zeros_like(grown)
        extra = [extra[0] + jnp.where(forward, grown, none), extra[1] + jnp.where(forward, none, grown)]
    if modes == 2:
        sums = table[z.lead : 2 * z.lead, :]
        both = by_head(z, three(states[0] * states[1]))
        decays = decays + jnp.sum(both, axis=1, keepdims=True) * jnp.exp(sums[:, -1:])
    steps_grad = steps_grad - rates[:, :1] * decays
    first = place[1] == 0
    half = z.rows
    early, late = total[:half, :].astype(BF16), total[half:, :].astype(BF16)
    own[...] = jnp.where(first, early, late)
    partner[:half, :] = jnp.where(first, late, early)
    early, late = steps_grad[:, :half], steps_grad[:, half:]
    grad_step[...] = jnp.where(first, early, late)
    partner[half:, :] = jnp.zeros((z.lead, z.width), BF16)
    high, low = two(jnp.where(first, late, early))
    partner[half:, :half] = high
    partner[half:, half : 2 * half] = low
    chunk = z.tokens // out.shape[0]
    for k in range(out.shape[0]):
        for which in range(2):
            share = extra[which][k * chunk : (k + 1) * chunk, :]
            power = exponent(share)
            out[k, which * chunk : (which + 1) * chunk, :] = share * jnp.exp2(-power)
            out[k, 2 * chunk + which : 2 * chunk + which + 1, :] = power
        out[k, 2 * chunk + 2 :, :] = jnp.zeros((6, z.state), F32)


def call(kernel, out_shape, scalars, arrays, flops, scratch=()):
    vmem = pl.BlockSpec(memory_space=pltpu.VMEM)
    smem = pl.BlockSpec(memory_space=pltpu.SMEM)
    return pl.pallas_call(
        kernel,
        out_shape=out_shape,
        in_specs=[smem] * len(scalars) + [vmem] * len(arrays),
        out_specs=[vmem] * len(out_shape),
        scratch_shapes=scratch,
        compiler_params=pltpu.CompilerParams(vmem_limit_bytes=40 * 1024 * 1024),
        cost_estimate=pl.CostEstimate(flops=flops, bytes_accessed=2_000_000, transcendentals=0),
    )(*scalars, *arrays)


def messages(z, peers, grad_out, step_sizes, x_ckpt, bc_ckpt):
    tokens = x_ckpt.shape[0]
    away = pl.BlockSpec(memory_space=pltpu.HBM)
    packed = (peers, tokens, z.width + 2 * z.state)
    return pl.pallas_call(
        partial(open_kernel, z),
        out_shape=[
            jax.ShapeDtypeStruct((z.rows + z.lead, z.width), BF16),
            jax.ShapeDtypeStruct(packed, BF16),
        ],
        in_specs=[away] * 4,
        out_specs=[away, away],
        scratch_shapes=[
            pltpu.VMEM(step_sizes.shape, F32),
            pltpu.VMEM(bc_ckpt.shape, BF16),
            pltpu.VMEM(packed, BF16),
            pltpu.VMEM((z.rows + z.lead, z.width), BF16),
            pltpu.SemaphoreType.DMA((4 + 2 * peers,)),
        ],
        compiler_params=pltpu.CompilerParams(vmem_limit_bytes=OPENING_VMEM),
    )(grad_out, step_sizes, x_ckpt, bc_ckpt)


def chain(state, passing, size, index, reverse):
    ring = [(i, i + 1) for i in range(size - 1)]
    if reverse:
        ring = [(j, i) for i, j in ring]
    place = size - 1 - index if reverse else index

    def hop(k, carry):
        entering, leaving = carry
        came = lax.ppermute(leaving, "pair", ring)
        here = place == k
        return (
            jnp.where(here, came, entering),
            jnp.where(here, passing * came + state, leaving),
        )

    return lax.fori_loop(1, size, hop, (jnp.zeros_like(state), state))[0]


def shards(x_ckpt, bc_ckpt, step_sizes, decay_rate, skip_gain, grad_out):
    heads, rows = step_sizes.shape
    z = Sizes(heads, rows, grad_out.shape[1], bc_ckpt.shape[2])
    pairs, tp = lax.axis_size("pair"), lax.axis_size("tp")
    pair, member = lax.axis_index("pair"), lax.axis_index("member")
    swap = [(0, 1), (1, 0)]
    modes = 1 if pairs == 2 else 2
    kinds = [pair] if modes == 1 else [jnp.int32(0), jnp.int32(1)]
    place = jnp.stack([pair, member, *kinds]).astype(jnp.int32)

    shape = jax.ShapeDtypeStruct
    tokens = x_ckpt.shape[0]
    message, slots = messages(z, 2 * tp, grad_out, step_sizes, x_ckpt, bc_ckpt)
    message = lax.ppermute(message, "member", swap)
    packed = lax.all_to_all(slots, ("member", "tp"), split_axis=0, concat_axis=0, tiled=True)
    packed = packed.reshape(z.tokens, z.width + 2 * z.state)

    mine = lax.dynamic_slice(decay_rate, (member * z.heads,), (z.heads,))
    rates = jnp.broadcast_to(jnp.pad(mine, (0, z.lead - z.heads))[:, None], (z.lead, LANES))
    mine = lax.dynamic_slice(skip_gain, (member * z.heads,), (z.heads,))
    gains = jnp.broadcast_to(jnp.repeat(mine, z.head_width)[None, :], (8, z.width))

    dy, table, scales = call(
        partial(prepare_kernel, z, modes),
        [
            shape((z.tokens, z.width), BF16),
            shape((2 * z.lead, z.tokens), F32),
            shape((modes, z.tokens, z.width), F32),
        ],
        [place],
        [step_sizes, message, rates, grad_out],
        1_000_000,
    )
    (state,) = call(
        partial(state_kernel, z, modes),
        [shape((modes, z.state_rows, LANES), F32)],
        [place],
        [packed, dy, table, scales],
        4 * z.tokens * z.state * z.width,
    )
    if modes == 1:
        turn = lax.ppermute(state.astype(jnp.float16), "pair", swap)
        came = turn.astype(F32)
    else:
        body = z.blocks * z.state
        passing = jnp.repeat(state[0, body : body + z.blocks], z.state, axis=0)
        forth = chain(state[0, :body], passing, pairs, pair, False)
        back = chain(state[1, :body], passing, pairs, pair, True)
        came = jnp.pad(jnp.stack([back, forth]), ((0, 0), (0, z.state_rows - body), (0, 0)))

    dx, gb, base, scaled = call(
        partial(local_kernel, z, modes),
        [
            shape((z.tokens, z.width), F32),
            shape((2, z.tokens, z.state), F32),
            shape((z.lead, z.tokens), F32),
            shape((2 * modes, z.tokens, z.width), BF16),
        ],
        [place],
        [packed, dy, table, scales, rates, gains],
        12 * z.tokens * z.tokens * z.width,
        [pltpu.VMEM((z.tokens, z.tokens), F32)],
    )
    out, own, partner, grad_step = call(
        partial(last_kernel, z, modes),
        [
            shape((2 * tp, 2 * tokens + 8, z.state), F32),
            shape((rows, z.width), BF16),
            shape((rows + z.lead, z.width), BF16),
            shape((z.lead, rows), F32),
        ],
        [place],
        [packed, table, scales, scaled, dx, base, gb, rates, came],
        12 * z.tokens * z.state * z.width,
    )
    swapped = lax.ppermute(partner, "member", swap)
    gathered = lax.all_to_all(
        out.astype(jnp.float16), ("member", "tp"), split_axis=0, concat_axis=0, tiled=True
    ).astype(F32)
    power = gathered[:, 2 * tokens : 2 * tokens + 2, None, :]
    parts = gathered[:, : 2 * tokens].reshape(2 * tp, 2, tokens, z.state)
    grad_bc = jnp.sum(parts * jnp.exp2(power), axis=0)
    first = member == 0
    theirs = swapped[:rows]
    grad_x = jnp.where(
        first,
        jnp.concatenate([own, theirs], axis=1),
        jnp.concatenate([theirs, own], axis=1),
    )
    tail = swapped[rows : rows + z.heads].astype(F32)
    theirs = tail[:, :rows] + tail[:, rows : 2 * rows]
    mine = grad_step[: z.heads]
    grad_step = jnp.where(
        first,
        jnp.concatenate([mine, theirs], axis=0),
        jnp.concatenate([theirs, mine], axis=0),
    )
    return (grad_x, grad_bc, grad_step)


def solution(mesh):
    sizes = dict(mesh.shape)
    names = []
    for name in mesh.axis_names:
        names += ["pair", "member"] if name == "seq" else [name]
    shape = []
    for name in mesh.axis_names:
        shape += [sizes[name] // 2, 2] if name == "seq" else [sizes[name]]
    fine = Mesh(mesh.devices.reshape(shape), tuple(names))
    seq = ("dp", "pair", "member")
    return jax.shard_map(
        shards,
        mesh=fine,
        in_specs=(
            P((*seq, "tp"), None),
            P(None, (*seq, "tp"), None),
            P("tp", seq),
            P("tp"),
            P("tp"),
            P(seq, "tp"),
        ),
        out_specs=(
            P(seq, "tp"),
            P(None, (*seq, "tp"), None),
            P("tp", seq),
        ),
        check_vma=False,
    )
```

```python
from functools import partial

import jax
import jax.numpy as jnp
from jax import lax
from jax.experimental import pallas as pl
from jax.experimental.pallas import tpu as pltpu
from jax.sharding import Mesh, PartitionSpec as P

F32 = jnp.float32
BF16 = jnp.bfloat16
LANES = 128
NEVER = -1e30
OPENING_VMEM = 66_800_000


def dot(a, b, dims=((1,), (0,))):
    return lax.dot_general(a, b, (dims, ((), ())), preferred_element_type=F32)


def two(a):
    high = a.astype(BF16)
    return high, (a - high.astype(F32)).astype(BF16)


def three(a):
    high = a.astype(BF16)
    rest = a - high.astype(F32)
    mid = rest.astype(BF16)
    return high, mid, (rest - mid.astype(F32)).astype(BF16)


def dots(parts, b, dims=((1,), (0,))):
    total = dot(parts[0], b, dims)
    for part in parts[1:]:
        total = total + dot(part, b, dims)
    return total


def below(rows, cols, test):
    i = lax.broadcasted_iota(jnp.int32, (rows, cols), 0)
    j = lax.broadcasted_iota(jnp.int32, (rows, cols), 1)
    return jnp.where(test(i, j), 1.0, 0.0).astype(BF16)


def lead(heads):
    return -(-heads // 16) * 16


class Sizes:
    def __init__(self, heads, rows, columns, state):
        self.heads = heads // 2
        self.rows = rows
        self.tokens = 2 * rows
        self.width = columns // 2
        self.head_width = self.width // self.heads
        self.state = state
        self.lead = lead(self.heads)
        self.blocks = self.width // LANES
        self.state_rows = self.blocks * state + -(-self.blocks // 8) * 8

    def spread(self):
        return below(self.lead, self.width, lambda i, j: j // self.head_width == i)


def exponent(a):
    top = jnp.max(jnp.abs(a), axis=0, keepdims=True)
    return jnp.ceil(jnp.log2(jnp.maximum(top, 1e-30)))


def by_head(z, parts):
    spread = z.spread()
    total = dot(spread, parts[0], ((1,), (1,)))
    for part in parts[1:]:
        total = total + dot(spread, part, ((1,), (1,)))
    return total


def tables(z, place, step, message, rates):
    first = place[1] == 0
    own = jnp.where(first, step[: z.heads, :], step[z.heads :, :])
    if z.lead > z.heads:
        own = jnp.concatenate([own, jnp.ones((z.lead - z.heads, z.rows), F32)], axis=0)
    tail = message[z.rows : z.rows + z.lead, : 3 * z.rows].astype(F32)
    other = tail[:, : z.rows] + tail[:, z.rows : 2 * z.rows] + tail[:, 2 * z.rows : 3 * z.rows]
    steps = jnp.concatenate([jnp.where(first, own, other), jnp.where(first, other, own)], axis=1)
    logs = steps * (-rates[:, :1])
    upto = below(z.tokens, z.tokens, lambda i, j: i <= j)
    return steps, dots(three(logs), upto)


def gradient(z, place, grad, message):
    first = place[1] == 0
    own = jnp.where(first, grad[:, : z.width], grad[:, z.width :])
    other = message[: z.rows, :]
    return jnp.concatenate([jnp.where(first, own, other), jnp.where(first, other, own)], axis=0)


def open_kernel(z, grad, step, x, bc, message, slots, held, shared, stage, note, sems):
    index = lax.axis_index("member")
    first = index == 0
    count = slots.shape[0]
    at = pl.multiple_of((1 - index) * z.width, LANES)
    sizes = pltpu.make_async_copy(step, held, sems.at[0])
    basis = pltpu.make_async_copy(bc, shared, sems.at[1])
    rows = pltpu.make_async_copy(grad.at[:, pl.ds(at, z.width)], note.at[pl.ds(0, z.rows), :], sems.at[2])
    sent = pltpu.make_async_copy(note, message, sems.at[3 + 2 * count])
    taken, given = [], []
    for k in range(count):
        member, peer = divmod(k, count // 2)
        columns = pl.ds((2 * peer + member) * z.width, z.width)
        taken.append(
            pltpu.make_async_copy(x.at[:, columns], stage.at[k, :, pl.ds(0, z.width)], sems.at[3 + k])
        )
        given.append(pltpu.make_async_copy(stage.at[k], slots.at[k], sems.at[3 + count + k]))
    for copy in (sizes, rows, basis, *taken):
        copy.start()
    note[z.rows :, :] = jnp.zeros((z.lead, z.width), BF16)
    sizes.wait()
    steps = jnp.where(first, held[z.heads :, :], held[: z.heads, :])
    if z.lead > z.heads:
        steps = jnp.concatenate([steps, jnp.ones((z.lead - z.heads, z.rows), F32)], axis=0)
    for k, part in enumerate(three(steps)):
        note[z.rows :, k * z.rows : (k + 1) * z.rows] = part
    rows.wait()
    sent.start()
    basis.wait()
    for k in range(count):
        stage[k, :, z.width : z.width + z.state] = shared[0]
        stage[k, :, z.width + z.state :] = shared[1]
    for k in range(count):
        taken[k].wait()
        given[k].start()
    for copy in (sent, *given):
        copy.wait()


def prepare_kernel(z, modes, place, step, message, rates, grad, dy, table, scales):
    steps, sums = tables(z, place, step, message, rates)
    dy[...] = gradient(z, place, grad, message)
    table[: z.lead, :] = steps
    table[z.lead : 2 * z.lead, :] = sums
    tail = steps * jnp.exp(sums[:, -1:] - sums)
    for k in range(modes):
        chosen = jnp.where(place[2 + k] == 0, tail, jnp.exp(sums))
        scales[k] = dots(three(chosen), z.spread(), ((0,), (0,)))


def weighted(z, forward, scale, packed, dy):
    source = jnp.where(forward, packed[:, : z.width], dy[...]).astype(F32)
    basis = jnp.where(
        forward,
        packed[:, z.width : z.width + z.state],
        packed[:, z.width + z.state :],
    )
    return scale * source, basis


def state_kernel(z, modes, place, packed, dy, table, scales, state):
    for k in range(modes):
        rows, basis = weighted(z, place[2 + k] == 0, scales[k], packed, dy)
        high, low = two(rows)
        found = dot(basis, high, ((0,), (0,))) + dot(basis, low, ((0,), (0,)))
        if modes == 1:
            power = exponent(found)
            found = found * jnp.exp2(-power)
        else:
            sums = table[z.lead : 2 * z.lead, :]
            passing = jnp.broadcast_to(jnp.exp(sums[:, -1:]), (z.lead, LANES))
            power = dots(three(passing), z.spread(), ((0,), (0,)))[:1, :]
        for block in range(z.blocks):
            at = slice(block * LANES, (block + 1) * LANES)
            state[k, block * z.state : (block + 1) * z.state, :] = found[:, at]
            state[k, z.blocks * z.state + block : z.blocks * z.state + block + 1, :] = power[:, at]
        left = state.shape[1] - z.blocks * (z.state + 1)
        if left:
            state[k, z.blocks * (z.state + 1) :, :] = jnp.zeros((left, LANES), F32)


def local_kernel(z, modes, place, packed, dy, table, scales, rates, gains, dx, gb, base, scaled, mixed):
    n, half = z.tokens, z.rows
    steps = table[: z.lead, :]
    sums = table[z.lead : 2 * z.lead, :]
    source = jnp.log(steps) - sums
    pad = jnp.zeros((LANES - z.lead, n), F32)
    columns = jnp.transpose(jnp.concatenate([source, pad], axis=0))
    b = packed[:, z.width : z.width + z.state]
    c = packed[:, z.width + z.state :]
    scores = dot(b, c, ((1,), (1,)))
    mixed[...] = jnp.zeros((n, n), F32)
    per = LANES // z.head_width
    lane = lax.broadcasted_iota(jnp.int32, (n, LANES), 1) // z.head_width
    read = []
    for block in range(z.width // LANES):
        at = slice(block * LANES, (block + 1) * LANES)
        values = packed[:, at]
        upstream = dy[:, at]
        total = jnp.zeros((n, LANES), F32)
        for k in range(per):
            h = block * per + k
            own = jnp.where(lane == k, upstream, jnp.zeros_like(upstream))
            row = sums[h : h + 1, :]
            pieces = []
            drawn = jnp.zeros((1, n), F32)
            for part in range(2):
                s = slice(part * half, (part + 1) * half)
                t = slice(part * half, n)
                wide = n - part * half
                i = lax.broadcasted_iota(jnp.int32, (half, wide), 0)
                j = lax.broadcasted_iota(jnp.int32, (half, wide), 1)
                gap = row[:, t] + columns[s, h : h + 1]
                decay = jnp.exp(jnp.where(j >= i, gap, NEVER))
                pairs = decay * dot(values[s, :], own[t, :], ((1,), (1,)))
                mixed[s, t] += pairs
                score = scores[s, t]
                seen = jnp.sum(pairs * score, axis=0, keepdims=True)
                if part:
                    seen = jnp.concatenate([jnp.zeros((1, half), F32), seen], axis=1)
                drawn = drawn + seen
                high, low = two(decay * score)
                pieces.append(dot(high, own[t, :]) + dot(low, own[t, :]))
            read.append(drawn)
            total = total + jnp.concatenate(pieces, axis=0)
        dx[:, at] = total
    seen = jnp.concatenate(read + [jnp.zeros((z.lead - z.heads, n), F32)], axis=0)
    given = by_head(z, two(packed[:, : z.width].astype(F32) * dx[...]))
    later = below(n, n, lambda i, j: i >= j)
    base[...] = given / steps - rates[:, :1] * dots(three(seen - given), later)
    dx[...] = dx[...] + gains[:1, :] * dy[...].astype(F32)
    high, low = two(mixed[...])
    gb[0] = dot(high, c) + dot(low, c)
    gb[1] = dot(high, b, ((0,), (0,))) + dot(low, b, ((0,), (0,)))
    for k in range(modes):
        rows, _ = weighted(z, place[2 + k] == 0, scales[k], packed, dy)
        high, low = two(rows)
        scaled[2 * k] = high
        scaled[2 * k + 1] = low


def arrived(z, state, k):
    parts = []
    for block in range(z.blocks):
        power = state[k, z.blocks * z.state + block : z.blocks * z.state + block + 1, :]
        parts.append(state[k, block * z.state : (block + 1) * z.state, :] * jnp.exp2(power))
    return jnp.concatenate(parts, axis=1)


def chosen(z, forward, packed):
    return jnp.where(
        forward,
        packed[:, z.width : z.width + z.state],
        packed[:, z.width + z.state :],
    )


def carry(basis, high, low):
    return dot(jnp.concatenate([basis, basis], axis=1), jnp.concatenate([high, low], axis=0))


def last_kernel(z, modes, place, packed, scales, scaled, dx, gb, state, out, own, partner):
    total = dx[...]
    extra = [gb[0], gb[1]]
    for k in range(modes):
        forward = place[2 + k] == 0
        high, low = two(arrived(z, state, k))
        carried = carry(chosen(z, forward, packed), high, low)
        total = total + jnp.where(forward, scales[k], jnp.zeros_like(carried)) * carried
        both = dot(scaled[2 * k], jnp.concatenate([high, low], axis=0), ((1,), (1,)))
        grown = both[:, : z.state] + both[:, z.state :] + dot(scaled[2 * k + 1], high, ((1,), (1,)))
        none = jnp.zeros_like(grown)
        extra = [extra[0] + jnp.where(forward, grown, none), extra[1] + jnp.where(forward, none, grown)]
    first = place[1] == 0
    half = z.rows
    early, late = total[:half, :].astype(BF16), total[half:, :].astype(BF16)
    own[...] = jnp.where(first, early, late)
    partner[...] = jnp.where(first, late, early)
    chunk = z.tokens // out.shape[0]
    for k in range(out.shape[0]):
        for which in range(2):
            out[k, which] = extra[which][k * chunk : (k + 1) * chunk, :]


def step_kernel(z, modes, place, packed, table, scaled, base, rates, state, own, partner):
    n = z.tokens
    steps = table[: z.lead, :]
    decays = jnp.zeros_like(steps)
    steps_grad = base[...]
    states = []
    for k in range(modes):
        forward = place[2 + k] == 0
        came = arrived(z, state, k)
        states.append(came)
        carried = carry(chosen(z, forward, packed), *two(came))
        rows = scaled[2 * k].astype(F32) + scaled[2 * k + 1].astype(F32)
        found = by_head(z, two(rows * carried))
        i = lax.broadcasted_iota(jnp.int32, (n, n), 0)
        j = lax.broadcasted_iota(jnp.int32, (n, n), 1)
        reach = (j - i) * jnp.where(forward, 1, -1) >= jnp.where(forward, 1, 0)
        decays = decays + dots(three(found), jnp.where(reach, 1.0, 0.0).astype(BF16))
        steps_grad = steps_grad + jnp.where(forward, found, jnp.zeros_like(found)) / steps
    if modes == 2:
        sums = table[z.lead : 2 * z.lead, :]
        both = by_head(z, three(states[0] * states[1]))
        decays = decays + jnp.sum(both, axis=1, keepdims=True) * jnp.exp(sums[:, -1:])
    steps_grad = steps_grad - rates[:, :1] * decays
    first = place[1] == 0
    early, late = steps_grad[:, : z.rows], steps_grad[:, z.rows :]
    own[...] = jnp.where(first, early, late)
    partner[...] = jnp.where(first, late, early)


def call(kernel, out_shape, scalars, arrays, flops, scratch=()):
    vmem = pl.BlockSpec(memory_space=pltpu.VMEM)
    smem = pl.BlockSpec(memory_space=pltpu.SMEM)
    return pl.pallas_call(
        kernel,
        out_shape=out_shape,
        in_specs=[smem] * len(scalars) + [vmem] * len(arrays),
        out_specs=[vmem] * len(out_shape),
        scratch_shapes=scratch,
        compiler_params=pltpu.CompilerParams(vmem_limit_bytes=40 * 1024 * 1024),
        cost_estimate=pl.CostEstimate(flops=flops, bytes_accessed=2_000_000, transcendentals=0),
    )(*scalars, *arrays)


def messages(z, peers, grad_out, step_sizes, x_ckpt, bc_ckpt):
    tokens = x_ckpt.shape[0]
    away = pl.BlockSpec(memory_space=pltpu.HBM)
    packed = (peers, tokens, z.width + 2 * z.state)
    return pl.pallas_call(
        partial(open_kernel, z),
        out_shape=[
            jax.ShapeDtypeStruct((z.rows + z.lead, z.width), BF16),
            jax.ShapeDtypeStruct(packed, BF16),
        ],
        in_specs=[away] * 4,
        out_specs=[away, away],
        scratch_shapes=[
            pltpu.VMEM(step_sizes.shape, F32),
            pltpu.VMEM(bc_ckpt.shape, BF16),
            pltpu.VMEM(packed, BF16),
            pltpu.VMEM((z.rows + z.lead, z.width), BF16),
            pltpu.SemaphoreType.DMA((4 + 2 * peers,)),
        ],
        compiler_params=pltpu.CompilerParams(vmem_limit_bytes=OPENING_VMEM),
    )(grad_out, step_sizes, x_ckpt, bc_ckpt)


def chain(state, passing, size, index, reverse):
    ring = [(i, i + 1) for i in range(size - 1)]
    if reverse:
        ring = [(j, i) for i, j in ring]
    place = size - 1 - index if reverse else index

    def hop(k, carry):
        entering, leaving = carry
        came = lax.ppermute(leaving, "pair", ring)
        here = place == k
        return (
            jnp.where(here, came, entering),
            jnp.where(here, passing * came + state, leaving),
        )

    return lax.fori_loop(1, size, hop, (jnp.zeros_like(state), state))[0]


def shards(x_ckpt, bc_ckpt, step_sizes, decay_rate, skip_gain, grad_out):
    heads, rows = step_sizes.shape
    z = Sizes(heads, rows, grad_out.shape[1], bc_ckpt.shape[2])
    pairs, tp = lax.axis_size("pair"), lax.axis_size("tp")
    pair, member = lax.axis_index("pair"), lax.axis_index("member")
    swap = [(0, 1), (1, 0)]
    modes = 1 if pairs == 2 else 2
    kinds = [pair] if modes == 1 else [jnp.int32(0), jnp.int32(1)]
    place = jnp.stack([pair, member, *kinds]).astype(jnp.int32)

    shape = jax.ShapeDtypeStruct
    tokens = x_ckpt.shape[0]
    message, slots = messages(z, 2 * tp, grad_out, step_sizes, x_ckpt, bc_ckpt)
    message = lax.ppermute(message, "member", swap)
    packed = lax.all_to_all(slots, ("member", "tp"), split_axis=0, concat_axis=0, tiled=True)
    packed = packed.reshape(z.tokens, z.width + 2 * z.state)

    mine = lax.dynamic_slice(decay_rate, (member * z.heads,), (z.heads,))
    rates = jnp.broadcast_to(jnp.pad(mine, (0, z.lead - z.heads))[:, None], (z.lead, LANES))
    mine = lax.dynamic_slice(skip_gain, (member * z.heads,), (z.heads,))
    gains = jnp.broadcast_to(jnp.repeat(mine, z.head_width)[None, :], (8, z.width))

    dy, table, scales = call(
        partial(prepare_kernel, z, modes),
        [
            shape((z.tokens, z.width), BF16),
            shape((2 * z.lead, z.tokens), F32),
            shape((modes, z.tokens, z.width), F32),
        ],
        [place],
        [step_sizes, message, rates, grad_out],
        1_000_000,
    )
    (state,) = call(
        partial(state_kernel, z, modes),
        [shape((modes, z.state_rows, LANES), F32)],
        [place],
        [packed, dy, table, scales],
        4 * z.tokens * z.state * z.width,
    )
    if modes == 1:
        turn = lax.ppermute(state.astype(jnp.float16), "pair", swap)
        came = turn.astype(F32)
    else:
        body = z.blocks * z.state
        passing = jnp.repeat(state[0, body : body + z.blocks], z.state, axis=0)
        forth = chain(state[0, :body], passing, pairs, pair, False)
        back = chain(state[1, :body], passing, pairs, pair, True)
        came = jnp.pad(jnp.stack([back, forth]), ((0, 0), (0, z.state_rows - body), (0, 0)))

    dx, gb, base, scaled = call(
        partial(local_kernel, z, modes),
        [
            shape((z.tokens, z.width), F32),
            shape((2, z.tokens, z.state), F32),
            shape((z.lead, z.tokens), F32),
            shape((2 * modes, z.tokens, z.width), BF16),
        ],
        [place],
        [packed, dy, table, scales, rates, gains],
        12 * z.tokens * z.tokens * z.width,
        [pltpu.VMEM((z.tokens, z.tokens), F32)],
    )
    out, own, partner = call(
        partial(last_kernel, z, modes),
        [
            shape((2 * tp, 2, tokens, z.state), F32),
            shape((rows, z.width), BF16),
            shape((rows, z.width), BF16),
        ],
        [place],
        [packed, scales, scaled, dx, gb, came],
        12 * z.tokens * z.state * z.width,
    )
    theirs = lax.ppermute(partner, "member", swap)
    gathered = lax.all_to_all(out, ("member", "tp"), split_axis=0, concat_axis=0, tiled=True)
    mine, partner = call(
        partial(step_kernel, z, modes),
        [shape((z.lead, rows), F32), shape((z.lead, rows), F32)],
        [place],
        [packed, table, scaled, base, rates, came],
        4 * z.tokens * z.state * z.width,
    )
    other = lax.ppermute(partner, "member", swap)
    grad_bc = jnp.sum(gathered, axis=0)
    first = member == 0
    grad_x = jnp.where(
        first,
        jnp.concatenate([own, theirs], axis=1),
        jnp.concatenate([theirs, own], axis=1),
    )
    mine, other = mine[: z.heads], other[: z.heads]
    grad_step = jnp.where(
        first,
        jnp.concatenate([mine, other], axis=0),
        jnp.concatenate([other, mine], axis=0),
    )
    return (grad_x, grad_bc, grad_step)


def solution(mesh):
    sizes = dict(mesh.shape)
    names = []
    for name in mesh.axis_names:
        names += ["pair", "member"] if name == "seq" else [name]
    shape = []
    for name in mesh.axis_names:
        shape += [sizes[name] // 2, 2] if name == "seq" else [sizes[name]]
    fine = Mesh(mesh.devices.reshape(shape), tuple(names))
    seq = ("dp", "pair", "member")
    return jax.shard_map(
        shards,
        mesh=fine,
        in_specs=(
            P((*seq, "tp"), None),
            P(None, (*seq, "tp"), None),
            P("tp", seq),
            P("tp"),
            P("tp"),
            P(seq, "tp"),
        ),
        out_specs=(
            P(seq, "tp"),
            P(None, (*seq, "tp"), None),
            P("tp", seq),
        ),
        check_vma=False,
    )
```

```python
from functools import partial

import jax
import jax.numpy as jnp
from jax import lax
from jax.experimental import pallas as pl
from jax.experimental.pallas import tpu as pltpu
from jax.sharding import Mesh, PartitionSpec as P

F32 = jnp.float32
BF16 = jnp.bfloat16
LANES = 128
NEVER = -1e30
OPENING_VMEM = 66_800_000


def dot(a, b, dims=((1,), (0,))):
    return lax.dot_general(a, b, (dims, ((), ())), preferred_element_type=F32)


def two(a):
    high = a.astype(BF16)
    return high, (a - high.astype(F32)).astype(BF16)


def three(a):
    high = a.astype(BF16)
    rest = a - high.astype(F32)
    mid = rest.astype(BF16)
    return high, mid, (rest - mid.astype(F32)).astype(BF16)


def dots(parts, b, dims=((1,), (0,))):
    total = dot(parts[0], b, dims)
    for part in parts[1:]:
        total = total + dot(part, b, dims)
    return total


def below(rows, cols, test):
    i = lax.broadcasted_iota(jnp.int32, (rows, cols), 0)
    j = lax.broadcasted_iota(jnp.int32, (rows, cols), 1)
    return jnp.where(test(i, j), 1.0, 0.0).astype(BF16)


def lead(heads):
    return -(-heads // 16) * 16


class Sizes:
    def __init__(self, heads, rows, columns, state):
        self.heads = heads // 2
        self.rows = rows
        self.tokens = 2 * rows
        self.width = columns // 2
        self.head_width = self.width // self.heads
        self.state = state
        self.lead = lead(self.heads)
        self.blocks = self.width // LANES
        self.state_rows = self.blocks * state + -(-self.blocks // 8) * 8

    def spread(self):
        return below(self.lead, self.width, lambda i, j: j // self.head_width == i)


def exponent(a):
    top = jnp.max(jnp.abs(a), axis=0, keepdims=True)
    return jnp.ceil(jnp.log2(jnp.maximum(top, 1e-30)))


def by_head(z, parts):
    spread = z.spread()
    total = dot(spread, parts[0], ((1,), (1,)))
    for part in parts[1:]:
        total = total + dot(spread, part, ((1,), (1,)))
    return total


def tables(z, place, step, message, rates):
    first = place[1] == 0
    own = jnp.where(first, step[: z.heads, :], step[z.heads :, :])
    if z.lead > z.heads:
        own = jnp.concatenate([own, jnp.ones((z.lead - z.heads, z.rows), F32)], axis=0)
    tail = message[z.rows : z.rows + z.lead, : 3 * z.rows].astype(F32)
    other = tail[:, : z.rows] + tail[:, z.rows : 2 * z.rows] + tail[:, 2 * z.rows : 3 * z.rows]
    steps = jnp.concatenate([jnp.where(first, own, other), jnp.where(first, other, own)], axis=1)
    logs = steps * (-rates[:, :1])
    upto = below(z.tokens, z.tokens, lambda i, j: i <= j)
    return steps, dots(three(logs), upto)


def gradient(z, place, grad, message):
    first = place[1] == 0
    own = jnp.where(first, grad[:, : z.width], grad[:, z.width :])
    other = message[: z.rows, :]
    return jnp.concatenate([jnp.where(first, own, other), jnp.where(first, other, own)], axis=0)


def open_kernel(z, grad, step, x, bc, message, slots, held, shared, stage, note, sems):
    index = lax.axis_index("member")
    first = index == 0
    count = slots.shape[0]
    at = pl.multiple_of((1 - index) * z.width, LANES)
    sizes = pltpu.make_async_copy(step, held, sems.at[0])
    basis = pltpu.make_async_copy(bc, shared, sems.at[1])
    rows = pltpu.make_async_copy(grad.at[:, pl.ds(at, z.width)], note.at[pl.ds(0, z.rows), :], sems.at[2])
    sent = pltpu.make_async_copy(note, message, sems.at[3 + 2 * count])
    taken, given = [], []
    for k in range(count):
        member, peer = divmod(k, count // 2)
        columns = pl.ds((2 * peer + member) * z.width, z.width)
        taken.append(
            pltpu.make_async_copy(x.at[:, columns], stage.at[k, :, pl.ds(0, z.width)], sems.at[3 + k])
        )
        given.append(pltpu.make_async_copy(stage.at[k], slots.at[k], sems.at[3 + count + k]))
    for copy in (sizes, rows, basis, *taken):
        copy.start()
    note[z.rows :, :] = jnp.zeros((z.lead, z.width), BF16)
    sizes.wait()
    steps = jnp.where(first, held[z.heads :, :], held[: z.heads, :])
    if z.lead > z.heads:
        steps = jnp.concatenate([steps, jnp.ones((z.lead - z.heads, z.rows), F32)], axis=0)
    for k, part in enumerate(three(steps)):
        note[z.rows :, k * z.rows : (k + 1) * z.rows] = part
    rows.wait()
    sent.start()
    basis.wait()
    for k in range(count):
        stage[k, :, z.width : z.width + z.state] = shared[0]
        stage[k, :, z.width + z.state :] = shared[1]
    for k in range(count):
        taken[k].wait()
        given[k].start()
    for copy in (sent, *given):
        copy.wait()


def prepare_kernel(z, modes, place, step, message, rates, grad, dy, table, scales):
    steps, sums = tables(z, place, step, message, rates)
    dy[...] = gradient(z, place, grad, message)
    table[: z.lead, :] = steps
    table[z.lead : 2 * z.lead, :] = sums
    tail = steps * jnp.exp(sums[:, -1:] - sums)
    for k in range(modes):
        chosen = jnp.where(place[2 + k] == 0, tail, jnp.exp(sums))
        scales[k] = dots(three(chosen), z.spread(), ((0,), (0,)))


def weighted(z, forward, scale, packed, dy):
    source = jnp.where(forward, packed[:, : z.width], dy[...]).astype(F32)
    basis = jnp.where(
        forward,
        packed[:, z.width : z.width + z.state],
        packed[:, z.width + z.state :],
    )
    return scale * source, basis


def state_kernel(z, modes, place, packed, dy, table, scales, state):
    for k in range(modes):
        rows, basis = weighted(z, place[2 + k] == 0, scales[k], packed, dy)
        high, low = two(rows)
        found = dot(basis, high, ((0,), (0,))) + dot(basis, low, ((0,), (0,)))
        if modes == 1:
            power = exponent(found)
            found = found * jnp.exp2(-power)
        else:
            sums = table[z.lead : 2 * z.lead, :]
            passing = jnp.broadcast_to(jnp.exp(sums[:, -1:]), (z.lead, LANES))
            power = dots(three(passing), z.spread(), ((0,), (0,)))[:1, :]
        for block in range(z.blocks):
            at = slice(block * LANES, (block + 1) * LANES)
            state[k, block * z.state : (block + 1) * z.state, :] = found[:, at]
            state[k, z.blocks * z.state + block : z.blocks * z.state + block + 1, :] = power[:, at]
        left = state.shape[1] - z.blocks * (z.state + 1)
        if left:
            state[k, z.blocks * (z.state + 1) :, :] = jnp.zeros((left, LANES), F32)


def local_kernel(z, modes, place, packed, dy, table, scales, rates, gains, dx, gb, base, scaled, mixed):
    n, half = z.tokens, z.rows
    steps = table[: z.lead, :]
    sums = table[z.lead : 2 * z.lead, :]
    source = jnp.log(steps) - sums
    pad = jnp.zeros((LANES - z.lead, n), F32)
    columns = jnp.transpose(jnp.concatenate([source, pad], axis=0))
    b = packed[:, z.width : z.width + z.state]
    c = packed[:, z.width + z.state :]
    scores = dot(b, c, ((1,), (1,)))
    mixed[...] = jnp.zeros((n, n), F32)
    per = LANES // z.head_width
    lane = lax.broadcasted_iota(jnp.int32, (n, LANES), 1) // z.head_width
    read = []
    for block in range(z.width // LANES):
        at = slice(block * LANES, (block + 1) * LANES)
        values = packed[:, at]
        upstream = dy[:, at]
        total = jnp.zeros((n, LANES), F32)
        for k in range(per):
            h = block * per + k
            own = jnp.where(lane == k, upstream, jnp.zeros_like(upstream))
            row = sums[h : h + 1, :]
            pieces = []
            drawn = jnp.zeros((1, n), F32)
            for part in range(2):
                s = slice(part * half, (part + 1) * half)
                t = slice(part * half, n)
                wide = n - part * half
                i = lax.broadcasted_iota(jnp.int32, (half, wide), 0)
                j = lax.broadcasted_iota(jnp.int32, (half, wide), 1)
                gap = row[:, t] + columns[s, h : h + 1]
                decay = jnp.exp(jnp.where(j >= i, gap, NEVER))
                pairs = decay * dot(values[s, :], own[t, :], ((1,), (1,)))
                mixed[s, t] += pairs
                score = scores[s, t]
                seen = jnp.sum(pairs * score, axis=0, keepdims=True)
                if part:
                    seen = jnp.concatenate([jnp.zeros((1, half), F32), seen], axis=1)
                drawn = drawn + seen
                high, low = two(decay * score)
                pieces.append(dot(high, own[t, :]) + dot(low, own[t, :]))
            read.append(drawn)
            total = total + jnp.concatenate(pieces, axis=0)
        dx[:, at] = total
    seen = jnp.concatenate(read + [jnp.zeros((z.lead - z.heads, n), F32)], axis=0)
    given = by_head(z, two(packed[:, : z.width].astype(F32) * dx[...]))
    later = below(n, n, lambda i, j: i >= j)
    base[...] = given / steps - rates[:, :1] * dots(three(seen - given), later)
    dx[...] = dx[...] + gains[:1, :] * dy[...].astype(F32)
    high, low = two(mixed[...])
    gb[0] = dot(high, c) + dot(low, c)
    gb[1] = dot(high, b, ((0,), (0,))) + dot(low, b, ((0,), (0,)))
    for k in range(modes):
        rows, _ = weighted(z, place[2 + k] == 0, scales[k], packed, dy)
        high, low = two(rows)
        scaled[2 * k] = high
        scaled[2 * k + 1] = low


def arrived(z, state, k):
    parts = []
    for block in range(z.blocks):
        power = state[k, z.blocks * z.state + block : z.blocks * z.state + block + 1, :]
        parts.append(state[k, block * z.state : (block + 1) * z.state, :] * jnp.exp2(power))
    return jnp.concatenate(parts, axis=1)


def chosen(z, forward, packed):
    return jnp.where(
        forward,
        packed[:, z.width : z.width + z.state],
        packed[:, z.width + z.state :],
    )


def carry(basis, high, low):
    return dot(jnp.concatenate([basis, basis], axis=1), jnp.concatenate([high, low], axis=0))


def last_kernel(z, modes, place, packed, scales, scaled, dx, gb, state, out, own, partner, stage, sem):
    extra = [gb[0], gb[1]]
    states = []
    for k in range(modes):
        forward = place[2 + k] == 0
        high, low = two(arrived(z, state, k))
        states.append((high, low))
        both = dot(scaled[2 * k], jnp.concatenate([high, low], axis=0), ((1,), (1,)))
        grown = both[:, : z.state] + both[:, z.state :] + dot(scaled[2 * k + 1], high, ((1,), (1,)))
        none = jnp.zeros_like(grown)
        extra = [extra[0] + jnp.where(forward, grown, none), extra[1] + jnp.where(forward, none, grown)]
    chunk = z.tokens // out.shape[0]
    for k in range(out.shape[0]):
        for which in range(2):
            stage[k, which] = extra[which][k * chunk : (k + 1) * chunk, :]
    shares = pltpu.make_async_copy(stage, out, sem)
    shares.start()
    total = dx[...]
    for k in range(modes):
        forward = place[2 + k] == 0
        carried = carry(chosen(z, forward, packed), *states[k])
        total = total + jnp.where(forward, scales[k], jnp.zeros_like(carried)) * carried
    first = place[1] == 0
    half = z.rows
    early, late = total[:half, :].astype(BF16), total[half:, :].astype(BF16)
    own[...] = jnp.where(first, early, late)
    partner[...] = jnp.where(first, late, early)
    shares.wait()


def step_kernel(z, modes, place, packed, table, scaled, base, rates, state, own, partner):
    n = z.tokens
    steps = table[: z.lead, :]
    decays = jnp.zeros_like(steps)
    steps_grad = base[...]
    states = []
    for k in range(modes):
        forward = place[2 + k] == 0
        came = arrived(z, state, k)
        states.append(came)
        carried = carry(chosen(z, forward, packed), *two(came))
        rows = scaled[2 * k].astype(F32) + scaled[2 * k + 1].astype(F32)
        found = by_head(z, two(rows * carried))
        i = lax.broadcasted_iota(jnp.int32, (n, n), 0)
        j = lax.broadcasted_iota(jnp.int32, (n, n), 1)
        reach = (j - i) * jnp.where(forward, 1, -1) >= jnp.where(forward, 1, 0)
        decays = decays + dots(three(found), jnp.where(reach, 1.0, 0.0).astype(BF16))
        steps_grad = steps_grad + jnp.where(forward, found, jnp.zeros_like(found)) / steps
    if modes == 2:
        sums = table[z.lead : 2 * z.lead, :]
        both = by_head(z, three(states[0] * states[1]))
        decays = decays + jnp.sum(both, axis=1, keepdims=True) * jnp.exp(sums[:, -1:])
    steps_grad = steps_grad - rates[:, :1] * decays
    first = place[1] == 0
    early, late = steps_grad[:, : z.rows], steps_grad[:, z.rows :]
    own[...] = jnp.where(first, early, late)
    partner[...] = jnp.where(first, late, early)


def call(kernel, out_shape, scalars, arrays, flops, scratch=(), away=0):
    vmem = pl.BlockSpec(memory_space=pltpu.VMEM)
    hbm = pl.BlockSpec(memory_space=pltpu.HBM)
    smem = pl.BlockSpec(memory_space=pltpu.SMEM)
    return pl.pallas_call(
        kernel,
        out_shape=out_shape,
        in_specs=[smem] * len(scalars) + [vmem] * len(arrays),
        out_specs=[hbm] * away + [vmem] * (len(out_shape) - away),
        scratch_shapes=scratch,
        compiler_params=pltpu.CompilerParams(vmem_limit_bytes=40 * 1024 * 1024),
        cost_estimate=pl.CostEstimate(flops=flops, bytes_accessed=2_000_000, transcendentals=0),
    )(*scalars, *arrays)


def messages(z, peers, grad_out, step_sizes, x_ckpt, bc_ckpt):
    tokens = x_ckpt.shape[0]
    away = pl.BlockSpec(memory_space=pltpu.HBM)
    packed = (peers, tokens, z.width + 2 * z.state)
    return pl.pallas_call(
        partial(open_kernel, z),
        out_shape=[
            jax.ShapeDtypeStruct((z.rows + z.lead, z.width), BF16),
            jax.ShapeDtypeStruct(packed, BF16),
        ],
        in_specs=[away] * 4,
        out_specs=[away, away],
        scratch_shapes=[
            pltpu.VMEM(step_sizes.shape, F32),
            pltpu.VMEM(bc_ckpt.shape, BF16),
            pltpu.VMEM(packed, BF16),
            pltpu.VMEM((z.rows + z.lead, z.width), BF16),
            pltpu.SemaphoreType.DMA((4 + 2 * peers,)),
        ],
        compiler_params=pltpu.CompilerParams(vmem_limit_bytes=OPENING_VMEM),
    )(grad_out, step_sizes, x_ckpt, bc_ckpt)


def chain(state, passing, size, index, reverse):
    ring = [(i, i + 1) for i in range(size - 1)]
    if reverse:
        ring = [(j, i) for i, j in ring]
    place = size - 1 - index if reverse else index

    def hop(k, carry):
        entering, leaving = carry
        came = lax.ppermute(leaving, "pair", ring)
        here = place == k
        return (
            jnp.where(here, came, entering),
            jnp.where(here, passing * came + state, leaving),
        )

    return lax.fori_loop(1, size, hop, (jnp.zeros_like(state), state))[0]


def shards(x_ckpt, bc_ckpt, step_sizes, decay_rate, skip_gain, grad_out):
    heads, rows = step_sizes.shape
    z = Sizes(heads, rows, grad_out.shape[1], bc_ckpt.shape[2])
    pairs, tp = lax.axis_size("pair"), lax.axis_size("tp")
    pair, member = lax.axis_index("pair"), lax.axis_index("member")
    swap = [(0, 1), (1, 0)]
    modes = 1 if pairs == 2 else 2
    kinds = [pair] if modes == 1 else [jnp.int32(0), jnp.int32(1)]
    place = jnp.stack([pair, member, *kinds]).astype(jnp.int32)

    shape = jax.ShapeDtypeStruct
    tokens = x_ckpt.shape[0]
    message, slots = messages(z, 2 * tp, grad_out, step_sizes, x_ckpt, bc_ckpt)
    message = lax.ppermute(message, "member", swap)
    packed = lax.all_to_all(slots, ("member", "tp"), split_axis=0, concat_axis=0, tiled=True)
    packed = packed.reshape(z.tokens, z.width + 2 * z.state)

    mine = lax.dynamic_slice(decay_rate, (member * z.heads,), (z.heads,))
    rates = jnp.broadcast_to(jnp.pad(mine, (0, z.lead - z.heads))[:, None], (z.lead, LANES))
    mine = lax.dynamic_slice(skip_gain, (member * z.heads,), (z.heads,))
    gains = jnp.broadcast_to(jnp.repeat(mine, z.head_width)[None, :], (8, z.width))

    dy, table, scales = call(
        partial(prepare_kernel, z, modes),
        [
            shape((z.tokens, z.width), BF16),
            shape((2 * z.lead, z.tokens), F32),
            shape((modes, z.tokens, z.width), F32),
        ],
        [place],
        [step_sizes, message, rates, grad_out],
        1_000_000,
    )
    (state,) = call(
        partial(state_kernel, z, modes),
        [shape((modes, z.state_rows, LANES), F32)],
        [place],
        [packed, dy, table, scales],
        4 * z.tokens * z.state * z.width,
    )
    if modes == 1:
        turn = lax.ppermute(state.astype(jnp.float16), "pair", swap)
        came = turn.astype(F32)
    else:
        body = z.blocks * z.state
        passing = jnp.repeat(state[0, body : body + z.blocks], z.state, axis=0)
        forth = chain(state[0, :body], passing, pairs, pair, False)
        back = chain(state[1, :body], passing, pairs, pair, True)
        came = jnp.pad(jnp.stack([back, forth]), ((0, 0), (0, z.state_rows - body), (0, 0)))

    dx, gb, base, scaled = call(
        partial(local_kernel, z, modes),
        [
            shape((z.tokens, z.width), F32),
            shape((2, z.tokens, z.state), F32),
            shape((z.lead, z.tokens), F32),
            shape((2 * modes, z.tokens, z.width), BF16),
        ],
        [place],
        [packed, dy, table, scales, rates, gains],
        12 * z.tokens * z.tokens * z.width,
        [pltpu.VMEM((z.tokens, z.tokens), F32)],
    )
    out, own, partner = call(
        partial(last_kernel, z, modes),
        [
            shape((2 * tp, 2, tokens, z.state), F32),
            shape((rows, z.width), BF16),
            shape((rows, z.width), BF16),
        ],
        [place],
        [packed, scales, scaled, dx, gb, came],
        12 * z.tokens * z.state * z.width,
        [pltpu.VMEM((2 * tp, 2, tokens, z.state), F32), pltpu.SemaphoreType.DMA],
        1,
    )
    theirs = lax.ppermute(partner, "member", swap)
    gathered = lax.all_to_all(out, ("member", "tp"), split_axis=0, concat_axis=0, tiled=True)
    mine, partner = call(
        partial(step_kernel, z, modes),
        [shape((z.lead, rows), F32), shape((z.lead, rows), F32)],
        [place],
        [packed, table, scaled, base, rates, came],
        4 * z.tokens * z.state * z.width,
    )
    other = lax.ppermute(partner, "member", swap)
    grad_bc = jnp.sum(gathered, axis=0)
    first = member == 0
    grad_x = jnp.where(
        first,
        jnp.concatenate([own, theirs], axis=1),
        jnp.concatenate([theirs, own], axis=1),
    )
    mine, other = mine[: z.heads], other[: z.heads]
    grad_step = jnp.where(
        first,
        jnp.concatenate([mine, other], axis=0),
        jnp.concatenate([other, mine], axis=0),
    )
    return (grad_x, grad_bc, grad_step)


def solution(mesh):
    sizes = dict(mesh.shape)
    names = []
    for name in mesh.axis_names:
        names += ["pair", "member"] if name == "seq" else [name]
    shape = []
    for name in mesh.axis_names:
        shape += [sizes[name] // 2, 2] if name == "seq" else [sizes[name]]
    fine = Mesh(mesh.devices.reshape(shape), tuple(names))
    seq = ("dp", "pair", "member")
    return jax.shard_map(
        shards,
        mesh=fine,
        in_specs=(
            P((*seq, "tp"), None),
            P(None, (*seq, "tp"), None),
            P("tp", seq),
            P("tp"),
            P("tp"),
            P(seq, "tp"),
        ),
        out_specs=(
            P(seq, "tp"),
            P(None, (*seq, "tp"), None),
            P("tp", seq),
        ),
        check_vma=False,
    )
```

```python
from functools import partial

import jax
import jax.numpy as jnp
from jax import lax
from jax.experimental import pallas as pl
from jax.experimental.pallas import tpu as pltpu
from jax.sharding import Mesh, PartitionSpec as P

F32 = jnp.float32
BF16 = jnp.bfloat16
LANES = 128
NEVER = -1e30
OPENING_VMEM = 66_800_000


def dot(a, b, dims=((1,), (0,))):
    return lax.dot_general(a, b, (dims, ((), ())), preferred_element_type=F32)


def two(a):
    high = a.astype(BF16)
    return high, (a - high.astype(F32)).astype(BF16)


def three(a):
    high = a.astype(BF16)
    rest = a - high.astype(F32)
    mid = rest.astype(BF16)
    return high, mid, (rest - mid.astype(F32)).astype(BF16)


def dots(parts, b, dims=((1,), (0,))):
    total = dot(parts[0], b, dims)
    for part in parts[1:]:
        total = total + dot(part, b, dims)
    return total


def below(rows, cols, test):
    i = lax.broadcasted_iota(jnp.int32, (rows, cols), 0)
    j = lax.broadcasted_iota(jnp.int32, (rows, cols), 1)
    return jnp.where(test(i, j), 1.0, 0.0).astype(BF16)


def lead(heads):
    return -(-heads // 16) * 16


class Sizes:
    def __init__(self, heads, rows, columns, state):
        self.heads = heads // 2
        self.rows = rows
        self.tokens = 2 * rows
        self.width = columns // 2
        self.head_width = self.width // self.heads
        self.state = state
        self.lead = lead(self.heads)
        self.blocks = self.width // LANES
        self.state_rows = self.blocks * state + -(-self.blocks // 8) * 8

    def spread(self):
        return below(self.lead, self.width, lambda i, j: j // self.head_width == i)


def onward(modes, k):
    return lax.axis_index("pair") == 0 if modes == 1 else k == 0


def exponent(a):
    top = jnp.max(jnp.abs(a), axis=0, keepdims=True)
    return jnp.ceil(jnp.log2(jnp.maximum(top, 1e-30)))


def by_head(z, parts):
    spread = z.spread()
    total = dot(spread, parts[0], ((1,), (1,)))
    for part in parts[1:]:
        total = total + dot(spread, part, ((1,), (1,)))
    return total


def tables(z, step, message, rates):
    first = lax.axis_index("member") == 0
    own = jnp.where(first, step[: z.heads, :], step[z.heads :, :])
    if z.lead > z.heads:
        own = jnp.concatenate([own, jnp.ones((z.lead - z.heads, z.rows), F32)], axis=0)
    tail = message[z.rows : z.rows + z.lead, : 3 * z.rows].astype(F32)
    other = tail[:, : z.rows] + tail[:, z.rows : 2 * z.rows] + tail[:, 2 * z.rows : 3 * z.rows]
    steps = jnp.concatenate([jnp.where(first, own, other), jnp.where(first, other, own)], axis=1)
    logs = steps * (-rates[:, :1])
    upto = below(z.tokens, z.tokens, lambda i, j: i <= j)
    return steps, dots(three(logs), upto)


def gradient(z, grad, message):
    first = lax.axis_index("member") == 0
    own = jnp.where(first, grad[:, : z.width], grad[:, z.width :])
    other = message[: z.rows, :]
    return jnp.concatenate([jnp.where(first, own, other), jnp.where(first, other, own)], axis=0)


def open_kernel(z, grad, step, x, bc, message, slots, held, shared, stage, note, sems):
    index = lax.axis_index("member")
    first = index == 0
    count = slots.shape[0]
    at = pl.multiple_of((1 - index) * z.width, LANES)
    sizes = pltpu.make_async_copy(step, held, sems.at[0])
    basis = pltpu.make_async_copy(bc, shared, sems.at[1])
    rows = pltpu.make_async_copy(grad.at[:, pl.ds(at, z.width)], note.at[pl.ds(0, z.rows), :], sems.at[2])
    sent = pltpu.make_async_copy(note, message, sems.at[3 + 2 * count])
    taken, given = [], []
    for k in range(count):
        member, peer = divmod(k, count // 2)
        columns = pl.ds((2 * peer + member) * z.width, z.width)
        taken.append(
            pltpu.make_async_copy(x.at[:, columns], stage.at[k, :, pl.ds(0, z.width)], sems.at[3 + k])
        )
        given.append(pltpu.make_async_copy(stage.at[k], slots.at[k], sems.at[3 + count + k]))
    for copy in (sizes, rows, basis, *taken):
        copy.start()
    note[z.rows :, :] = jnp.zeros((z.lead, z.width), BF16)
    sizes.wait()
    steps = jnp.where(first, held[z.heads :, :], held[: z.heads, :])
    if z.lead > z.heads:
        steps = jnp.concatenate([steps, jnp.ones((z.lead - z.heads, z.rows), F32)], axis=0)
    for k, part in enumerate(three(steps)):
        note[z.rows :, k * z.rows : (k + 1) * z.rows] = part
    rows.wait()
    sent.start()
    basis.wait()
    for k in range(count):
        stage[k, :, z.width : z.width + z.state] = shared[0]
        stage[k, :, z.width + z.state :] = shared[1]
    for k in range(count):
        taken[k].wait()
        given[k].start()
    for copy in (sent, *given):
        copy.wait()


def prepare_kernel(z, modes, step, message, rates, grad, dy, table, scales):
    steps, sums = tables(z, step, message, rates)
    dy[...] = gradient(z, grad, message)
    table[: z.lead, :] = steps
    table[z.lead : 2 * z.lead, :] = sums
    tail = steps * jnp.exp(sums[:, -1:] - sums)
    for k in range(modes):
        chosen = jnp.where(onward(modes, k), tail, jnp.exp(sums))
        scales[k] = dots(three(chosen), z.spread(), ((0,), (0,)))


def weighted(z, forward, scale, packed, dy):
    source = jnp.where(forward, packed[:, : z.width], dy[...]).astype(F32)
    basis = jnp.where(
        forward,
        packed[:, z.width : z.width + z.state],
        packed[:, z.width + z.state :],
    )
    return scale * source, basis


def state_kernel(z, modes, packed, dy, table, scales, state):
    for k in range(modes):
        rows, basis = weighted(z, onward(modes, k), scales[k], packed, dy)
        high, low = two(rows)
        found = dot(basis, high, ((0,), (0,))) + dot(basis, low, ((0,), (0,)))
        if modes == 1:
            power = exponent(found)
            found = found * jnp.exp2(-power)
        else:
            sums = table[z.lead : 2 * z.lead, :]
            passing = jnp.broadcast_to(jnp.exp(sums[:, -1:]), (z.lead, LANES))
            power = dots(three(passing), z.spread(), ((0,), (0,)))[:1, :]
        for block in range(z.blocks):
            at = slice(block * LANES, (block + 1) * LANES)
            state[k, block * z.state : (block + 1) * z.state, :] = found[:, at]
            state[k, z.blocks * z.state + block : z.blocks * z.state + block + 1, :] = power[:, at]
        left = state.shape[1] - z.blocks * (z.state + 1)
        if left:
            state[k, z.blocks * (z.state + 1) :, :] = jnp.zeros((left, LANES), F32)


def local_kernel(z, modes, packed, dy, table, scales, rates, gains, dx, gb, base, scaled, mixed):
    n, half = z.tokens, z.rows
    steps = table[: z.lead, :]
    sums = table[z.lead : 2 * z.lead, :]
    source = jnp.log(steps) - sums
    pad = jnp.zeros((LANES - z.lead, n), F32)
    columns = jnp.transpose(jnp.concatenate([source, pad], axis=0))
    b = packed[:, z.width : z.width + z.state]
    c = packed[:, z.width + z.state :]
    scores = dot(b, c, ((1,), (1,)))
    mixed[...] = jnp.zeros((n, n), F32)
    per = LANES // z.head_width
    lane = lax.broadcasted_iota(jnp.int32, (n, LANES), 1) // z.head_width
    read = []
    for block in range(z.width // LANES):
        at = slice(block * LANES, (block + 1) * LANES)
        values = packed[:, at]
        upstream = dy[:, at]
        total = jnp.zeros((n, LANES), F32)
        for k in range(per):
            h = block * per + k
            own = jnp.where(lane == k, upstream, jnp.zeros_like(upstream))
            row = sums[h : h + 1, :]
            pieces = []
            drawn = jnp.zeros((1, n), F32)
            for part in range(2):
                s = slice(part * half, (part + 1) * half)
                t = slice(part * half, n)
                wide = n - part * half
                i = lax.broadcasted_iota(jnp.int32, (half, wide), 0)
                j = lax.broadcasted_iota(jnp.int32, (half, wide), 1)
                gap = row[:, t] + columns[s, h : h + 1]
                decay = jnp.exp(jnp.where(j >= i, gap, NEVER))
                pairs = decay * dot(values[s, :], own[t, :], ((1,), (1,)))
                mixed[s, t] += pairs
                score = scores[s, t]
                seen = jnp.sum(pairs * score, axis=0, keepdims=True)
                if part:
                    seen = jnp.concatenate([jnp.zeros((1, half), F32), seen], axis=1)
                drawn = drawn + seen
                high, low = two(decay * score)
                pieces.append(dot(high, own[t, :]) + dot(low, own[t, :]))
            read.append(drawn)
            total = total + jnp.concatenate(pieces, axis=0)
        dx[:, at] = total
    seen = jnp.concatenate(read + [jnp.zeros((z.lead - z.heads, n), F32)], axis=0)
    given = by_head(z, two(packed[:, : z.width].astype(F32) * dx[...]))
    later = below(n, n, lambda i, j: i >= j)
    base[...] = given / steps - rates[:, :1] * dots(three(seen - given), later)
    dx[...] = dx[...] + gains[:1, :] * dy[...].astype(F32)
    high, low = two(mixed[...])
    gb[0] = dot(high, c) + dot(low, c)
    gb[1] = dot(high, b, ((0,), (0,))) + dot(low, b, ((0,), (0,)))
    for k in range(modes):
        rows, _ = weighted(z, onward(modes, k), scales[k], packed, dy)
        high, low = two(rows)
        scaled[2 * k] = high
        scaled[2 * k + 1] = low


def arrived(z, state, k):
    parts = []
    for block in range(z.blocks):
        power = state[k, z.blocks * z.state + block : z.blocks * z.state + block + 1, :]
        parts.append(state[k, block * z.state : (block + 1) * z.state, :] * jnp.exp2(power))
    return jnp.concatenate(parts, axis=1)


def chosen(z, forward, packed):
    return jnp.where(
        forward,
        packed[:, z.width : z.width + z.state],
        packed[:, z.width + z.state :],
    )


def carry(basis, high, low):
    return dot(jnp.concatenate([basis, basis], axis=1), jnp.concatenate([high, low], axis=0))


def last_kernel(z, modes, packed, scales, scaled, dx, gb, state, out, own, partner, stage, sem):
    extra = [gb[0], gb[1]]
    states = []
    for k in range(modes):
        forward = onward(modes, k)
        high, low = two(arrived(z, state, k))
        states.append((high, low))
        both = dot(scaled[2 * k], jnp.concatenate([high, low], axis=0), ((1,), (1,)))
        grown = both[:, : z.state] + both[:, z.state :] + dot(scaled[2 * k + 1], high, ((1,), (1,)))
        none = jnp.zeros_like(grown)
        extra = [extra[0] + jnp.where(forward, grown, none), extra[1] + jnp.where(forward, none, grown)]
    chunk = z.tokens // out.shape[0]
    for k in range(out.shape[0]):
        for which in range(2):
            stage[k, which] = extra[which][k * chunk : (k + 1) * chunk, :]
    shares = pltpu.make_async_copy(stage, out, sem)
    shares.start()
    total = dx[...]
    for k in range(modes):
        forward = onward(modes, k)
        carried = carry(chosen(z, forward, packed), *states[k])
        total = total + jnp.where(forward, scales[k], jnp.zeros_like(carried)) * carried
    first = lax.axis_index("member") == 0
    half = z.rows
    early, late = total[:half, :].astype(BF16), total[half:, :].astype(BF16)
    own[...] = jnp.where(first, early, late)
    partner[...] = jnp.where(first, late, early)
    shares.wait()


def step_kernel(z, modes, packed, table, scaled, base, rates, state, own, partner):
    n = z.tokens
    steps = table[: z.lead, :]
    decays = jnp.zeros_like(steps)
    steps_grad = base[...]
    states = []
    for k in range(modes):
        forward = onward(modes, k)
        came = arrived(z, state, k)
        states.append(came)
        carried = carry(chosen(z, forward, packed), *two(came))
        rows = scaled[2 * k].astype(F32) + scaled[2 * k + 1].astype(F32)
        found = by_head(z, two(rows * carried))
        i = lax.broadcasted_iota(jnp.int32, (n, n), 0)
        j = lax.broadcasted_iota(jnp.int32, (n, n), 1)
        reach = (j - i) * jnp.where(forward, 1, -1) >= jnp.where(forward, 1, 0)
        decays = decays + dots(three(found), jnp.where(reach, 1.0, 0.0).astype(BF16))
        steps_grad = steps_grad + jnp.where(forward, found, jnp.zeros_like(found)) / steps
    if modes == 2:
        sums = table[z.lead : 2 * z.lead, :]
        both = by_head(z, three(states[0] * states[1]))
        decays = decays + jnp.sum(both, axis=1, keepdims=True) * jnp.exp(sums[:, -1:])
    steps_grad = steps_grad - rates[:, :1] * decays
    first = lax.axis_index("member") == 0
    early, late = steps_grad[:, : z.rows], steps_grad[:, z.rows :]
    own[...] = jnp.where(first, early, late)
    partner[...] = jnp.where(first, late, early)


def call(kernel, out_shape, arrays, flops, scratch=(), away=0):
    vmem = pl.BlockSpec(memory_space=pltpu.VMEM)
    hbm = pl.BlockSpec(memory_space=pltpu.HBM)
    return pl.pallas_call(
        kernel,
        out_shape=out_shape,
        in_specs=[vmem] * len(arrays),
        out_specs=[hbm] * away + [vmem] * (len(out_shape) - away),
        scratch_shapes=scratch,
        compiler_params=pltpu.CompilerParams(vmem_limit_bytes=40 * 1024 * 1024),
        cost_estimate=pl.CostEstimate(flops=flops, bytes_accessed=2_000_000, transcendentals=0),
    )(*arrays)


def messages(z, peers, grad_out, step_sizes, x_ckpt, bc_ckpt):
    tokens = x_ckpt.shape[0]
    away = pl.BlockSpec(memory_space=pltpu.HBM)
    packed = (peers, tokens, z.width + 2 * z.state)
    return pl.pallas_call(
        partial(open_kernel, z),
        out_shape=[
            jax.ShapeDtypeStruct((z.rows + z.lead, z.width), BF16),
            jax.ShapeDtypeStruct(packed, BF16),
        ],
        in_specs=[away] * 4,
        out_specs=[away, away],
        scratch_shapes=[
            pltpu.VMEM(step_sizes.shape, F32),
            pltpu.VMEM(bc_ckpt.shape, BF16),
            pltpu.VMEM(packed, BF16),
            pltpu.VMEM((z.rows + z.lead, z.width), BF16),
            pltpu.SemaphoreType.DMA((4 + 2 * peers,)),
        ],
        compiler_params=pltpu.CompilerParams(vmem_limit_bytes=OPENING_VMEM),
    )(grad_out, step_sizes, x_ckpt, bc_ckpt)


def chain(state, passing, size, index, reverse):
    ring = [(i, i + 1) for i in range(size - 1)]
    if reverse:
        ring = [(j, i) for i, j in ring]
    place = size - 1 - index if reverse else index

    def hop(k, carry):
        entering, leaving = carry
        came = lax.ppermute(leaving, "pair", ring)
        here = place == k
        return (
            jnp.where(here, came, entering),
            jnp.where(here, passing * came + state, leaving),
        )

    return lax.fori_loop(1, size, hop, (jnp.zeros_like(state), state))[0]


def shards(x_ckpt, bc_ckpt, step_sizes, decay_rate, skip_gain, grad_out):
    heads, rows = step_sizes.shape
    z = Sizes(heads, rows, grad_out.shape[1], bc_ckpt.shape[2])
    pairs, tp = lax.axis_size("pair"), lax.axis_size("tp")
    pair, member = lax.axis_index("pair"), lax.axis_index("member")
    swap = [(0, 1), (1, 0)]
    modes = 1 if pairs == 2 else 2

    shape = jax.ShapeDtypeStruct
    tokens = x_ckpt.shape[0]
    message, slots = messages(z, 2 * tp, grad_out, step_sizes, x_ckpt, bc_ckpt)
    message = lax.ppermute(message, "member", swap)
    packed = lax.all_to_all(slots, ("member", "tp"), split_axis=0, concat_axis=0, tiled=True)
    packed = packed.reshape(z.tokens, z.width + 2 * z.state)

    mine = lax.dynamic_slice(decay_rate, (member * z.heads,), (z.heads,))
    rates = jnp.broadcast_to(jnp.pad(mine, (0, z.lead - z.heads))[:, None], (z.lead, LANES))
    mine = lax.dynamic_slice(skip_gain, (member * z.heads,), (z.heads,))
    gains = jnp.broadcast_to(jnp.repeat(mine, z.head_width)[None, :], (8, z.width))

    dy, table, scales = call(
        partial(prepare_kernel, z, modes),
        [
            shape((z.tokens, z.width), BF16),
            shape((2 * z.lead, z.tokens), F32),
            shape((modes, z.tokens, z.width), F32),
        ],
        [step_sizes, message, rates, grad_out],
        1_000_000,
    )
    (state,) = call(
        partial(state_kernel, z, modes),
        [shape((modes, z.state_rows, LANES), F32)],
        [packed, dy, table, scales],
        4 * z.tokens * z.state * z.width,
    )
    if modes == 1:
        turn = lax.ppermute(state.astype(jnp.float16), "pair", swap)
        came = turn.astype(F32)
    else:
        body = z.blocks * z.state
        passing = jnp.repeat(state[0, body : body + z.blocks], z.state, axis=0)
        forth = chain(state[0, :body], passing, pairs, pair, False)
        back = chain(state[1, :body], passing, pairs, pair, True)
        came = jnp.pad(jnp.stack([back, forth]), ((0, 0), (0, z.state_rows - body), (0, 0)))

    dx, gb, base, scaled = call(
        partial(local_kernel, z, modes),
        [
            shape((z.tokens, z.width), F32),
            shape((2, z.tokens, z.state), F32),
            shape((z.lead, z.tokens), F32),
            shape((2 * modes, z.tokens, z.width), BF16),
        ],
        [packed, dy, table, scales, rates, gains],
        12 * z.tokens * z.tokens * z.width,
        [pltpu.VMEM((z.tokens, z.tokens), F32)],
    )
    out, own, partner = call(
        partial(last_kernel, z, modes),
        [
            shape((2 * tp, 2, tokens, z.state), F32),
            shape((rows, z.width), BF16),
            shape((rows, z.width), BF16),
        ],
        [packed, scales, scaled, dx, gb, came],
        12 * z.tokens * z.state * z.width,
        [pltpu.VMEM((2 * tp, 2, tokens, z.state), F32), pltpu.SemaphoreType.DMA],
        1,
    )
    theirs = lax.ppermute(partner, "member", swap)
    gathered = lax.all_to_all(out, ("member", "tp"), split_axis=0, concat_axis=0, tiled=True)
    mine, partner = call(
        partial(step_kernel, z, modes),
        [shape((z.lead, rows), F32), shape((z.lead, rows), F32)],
        [packed, table, scaled, base, rates, came],
        4 * z.tokens * z.state * z.width,
    )
    other = lax.ppermute(partner, "member", swap)
    grad_bc = jnp.sum(gathered, axis=0)
    first = member == 0
    grad_x = jnp.where(
        first,
        jnp.concatenate([own, theirs], axis=1),
        jnp.concatenate([theirs, own], axis=1),
    )
    mine, other = mine[: z.heads], other[: z.heads]
    grad_step = jnp.where(
        first,
        jnp.concatenate([mine, other], axis=0),
        jnp.concatenate([other, mine], axis=0),
    )
    return (grad_x, grad_bc, grad_step)


def solution(mesh):
    sizes = dict(mesh.shape)
    names = []
    for name in mesh.axis_names:
        names += ["pair", "member"] if name == "seq" else [name]
    shape = []
    for name in mesh.axis_names:
        shape += [sizes[name] // 2, 2] if name == "seq" else [sizes[name]]
    fine = Mesh(mesh.devices.reshape(shape), tuple(names))
    seq = ("dp", "pair", "member")
    return jax.shard_map(
        shards,
        mesh=fine,
        in_specs=(
            P((*seq, "tp"), None),
            P(None, (*seq, "tp"), None),
            P("tp", seq),
            P("tp"),
            P("tp"),
            P(seq, "tp"),
        ),
        out_specs=(
            P(seq, "tp"),
            P(None, (*seq, "tp"), None),
            P("tp", seq),
        ),
        check_vma=False,
    )
```

```python
from functools import partial

import jax
import jax.numpy as jnp
from jax import lax
from jax.experimental import pallas as pl
from jax.experimental.pallas import tpu as pltpu
from jax.sharding import Mesh, PartitionSpec as P

F32 = jnp.float32
BF16 = jnp.bfloat16
LANES = 128
NEVER = -1e30
OPENING_VMEM = 66_800_000


def dot(a, b, dims=((1,), (0,))):
    return lax.dot_general(a, b, (dims, ((), ())), preferred_element_type=F32)


def two(a):
    high = a.astype(BF16)
    return high, (a - high.astype(F32)).astype(BF16)


def three(a):
    high = a.astype(BF16)
    rest = a - high.astype(F32)
    mid = rest.astype(BF16)
    return high, mid, (rest - mid.astype(F32)).astype(BF16)


def dots(parts, b, dims=((1,), (0,))):
    total = dot(parts[0], b, dims)
    for part in parts[1:]:
        total = total + dot(part, b, dims)
    return total


def below(rows, cols, test):
    i = lax.broadcasted_iota(jnp.int32, (rows, cols), 0)
    j = lax.broadcasted_iota(jnp.int32, (rows, cols), 1)
    return jnp.where(test(i, j), 1.0, 0.0).astype(BF16)


def lead(heads):
    return -(-heads // 16) * 16


class Sizes:
    def __init__(self, heads, rows, columns, state):
        self.heads = heads // 2
        self.rows = rows
        self.tokens = 2 * rows
        self.width = columns // 2
        self.head_width = self.width // self.heads
        self.state = state
        self.lead = lead(self.heads)
        self.blocks = self.width // LANES
        self.state_rows = self.blocks * state + -(-self.blocks // 8) * 8

    def spread(self):
        return below(self.lead, self.width, lambda i, j: j // self.head_width == i)


def onward(modes, k):
    return lax.axis_index("pair") == 0 if modes == 1 else k == 0


def exponent(a):
    top = jnp.max(jnp.abs(a), axis=0, keepdims=True)
    return jnp.ceil(jnp.log2(jnp.maximum(top, 1e-30)))


def by_head(z, parts):
    spread = z.spread()
    total = dot(spread, parts[0], ((1,), (1,)))
    for part in parts[1:]:
        total = total + dot(spread, part, ((1,), (1,)))
    return total


def tables(z, step, message, rates):
    first = lax.axis_index("member") == 0
    own = jnp.where(first, step[: z.heads, :], step[z.heads :, :])
    if z.lead > z.heads:
        own = jnp.concatenate([own, jnp.ones((z.lead - z.heads, z.rows), F32)], axis=0)
    tail = message[z.rows : z.rows + z.lead, : 3 * z.rows].astype(F32)
    other = tail[:, : z.rows] + tail[:, z.rows : 2 * z.rows] + tail[:, 2 * z.rows : 3 * z.rows]
    steps = jnp.concatenate([jnp.where(first, own, other), jnp.where(first, other, own)], axis=1)
    logs = steps * (-rates[:, :1])
    upto = below(z.tokens, z.tokens, lambda i, j: i <= j)
    return steps, dots(three(logs), upto)


def gradient(z, grad, message):
    first = lax.axis_index("member") == 0
    own = jnp.where(first, grad[:, : z.width], grad[:, z.width :])
    other = message[: z.rows, :]
    return jnp.concatenate([jnp.where(first, own, other), jnp.where(first, other, own)], axis=0)


def open_kernel(z, grad, step, x, bc, message, slots, held, shared, stage, note, sems):
    index = lax.axis_index("member")
    first = index == 0
    count = slots.shape[0]
    at = pl.multiple_of((1 - index) * z.width, LANES)
    sizes = pltpu.make_async_copy(step, held, sems.at[0])
    rows = pltpu.make_async_copy(grad.at[:, pl.ds(at, z.width)], note.at[pl.ds(0, z.rows), :], sems.at[1])
    basis = pltpu.make_async_copy(bc, shared, sems.at[2])
    channels = stage.at[:, :, pl.ds(0, z.width)]
    every = pltpu.make_async_copy(channels, channels, sems.at[3])
    sent = pltpu.make_async_copy(note, message, sems.at[4])
    given = pltpu.make_async_copy(stage, slots, sems.at[5])
    rows.start()
    for k in range(count):
        member, peer = divmod(k, count // 2)
        columns = pl.ds((2 * peer + member) * z.width, z.width)
        pltpu.make_async_copy(x.at[:, columns], stage.at[k, :, pl.ds(0, z.width)], sems.at[3]).start()
    basis.start()
    sizes.start()
    note[z.rows :, :] = jnp.zeros((z.lead, z.width), BF16)
    basis.wait()
    for k in range(count):
        stage[k, :, z.width : z.width + z.state] = shared[0]
        stage[k, :, z.width + z.state :] = shared[1]
    sizes.wait()
    steps = jnp.where(first, held[z.heads :, :], held[: z.heads, :])
    if z.lead > z.heads:
        steps = jnp.concatenate([steps, jnp.ones((z.lead - z.heads, z.rows), F32)], axis=0)
    for k, part in enumerate(three(steps)):
        note[z.rows :, k * z.rows : (k + 1) * z.rows] = part
    every.wait()
    given.start()
    rows.wait()
    sent.start()
    sent.wait()
    given.wait()


def prepare_kernel(z, modes, step, message, rates, grad, dy, table, scales):
    steps, sums = tables(z, step, message, rates)
    dy[...] = gradient(z, grad, message)
    table[: z.lead, :] = steps
    table[z.lead : 2 * z.lead, :] = sums
    tail = steps * jnp.exp(sums[:, -1:] - sums)
    for k in range(modes):
        chosen = jnp.where(onward(modes, k), tail, jnp.exp(sums))
        scales[k] = dots(three(chosen), z.spread(), ((0,), (0,)))


def weighted(z, forward, scale, packed, dy):
    source = jnp.where(forward, packed[:, : z.width], dy[...]).astype(F32)
    basis = jnp.where(
        forward,
        packed[:, z.width : z.width + z.state],
        packed[:, z.width + z.state :],
    )
    return scale * source, basis


def state_kernel(z, modes, packed, dy, table, scales, state):
    for k in range(modes):
        rows, basis = weighted(z, onward(modes, k), scales[k], packed, dy)
        high, low = two(rows)
        found = dot(basis, high, ((0,), (0,))) + dot(basis, low, ((0,), (0,)))
        if modes == 1:
            power = exponent(found)
            found = found * jnp.exp2(-power)
        else:
            sums = table[z.lead : 2 * z.lead, :]
            passing = jnp.broadcast_to(jnp.exp(sums[:, -1:]), (z.lead, LANES))
            power = dots(three(passing), z.spread(), ((0,), (0,)))[:1, :]
        for block in range(z.blocks):
            at = slice(block * LANES, (block + 1) * LANES)
            state[k, block * z.state : (block + 1) * z.state, :] = found[:, at]
            state[k, z.blocks * z.state + block : z.blocks * z.state + block + 1, :] = power[:, at]
        left = state.shape[1] - z.blocks * (z.state + 1)
        if left:
            state[k, z.blocks * (z.state + 1) :, :] = jnp.zeros((left, LANES), F32)


def local_kernel(z, modes, packed, dy, table, scales, rates, gains, dx, gb, base, scaled, mixed):
    n, half = z.tokens, z.rows
    steps = table[: z.lead, :]
    sums = table[z.lead : 2 * z.lead, :]
    source = jnp.log(steps) - sums
    pad = jnp.zeros((LANES - z.lead, n), F32)
    columns = jnp.transpose(jnp.concatenate([source, pad], axis=0))
    b = packed[:, z.width : z.width + z.state]
    c = packed[:, z.width + z.state :]
    scores = dot(b, c, ((1,), (1,)))
    mixed[...] = jnp.zeros((n, n), F32)
    per = LANES // z.head_width
    lane = lax.broadcasted_iota(jnp.int32, (n, LANES), 1) // z.head_width
    read = []
    for block in range(z.width // LANES):
        at = slice(block * LANES, (block + 1) * LANES)
        values = packed[:, at]
        upstream = dy[:, at]
        total = jnp.zeros((n, LANES), F32)
        for k in range(per):
            h = block * per + k
            own = jnp.where(lane == k, upstream, jnp.zeros_like(upstream))
            row = sums[h : h + 1, :]
            pieces = []
            drawn = jnp.zeros((1, n), F32)
            for part in range(2):
                s = slice(part * half, (part + 1) * half)
                t = slice(part * half, n)
                wide = n - part * half
                i = lax.broadcasted_iota(jnp.int32, (half, wide), 0)
                j = lax.broadcasted_iota(jnp.int32, (half, wide), 1)
                gap = row[:, t] + columns[s, h : h + 1]
                decay = jnp.exp(jnp.where(j >= i, gap, NEVER))
                pairs = decay * dot(values[s, :], own[t, :], ((1,), (1,)))
                mixed[s, t] += pairs
                score = scores[s, t]
                seen = jnp.sum(pairs * score, axis=0, keepdims=True)
                if part:
                    seen = jnp.concatenate([jnp.zeros((1, half), F32), seen], axis=1)
                drawn = drawn + seen
                high, low = two(decay * score)
                pieces.append(dot(high, own[t, :]) + dot(low, own[t, :]))
            read.append(drawn)
            total = total + jnp.concatenate(pieces, axis=0)
        dx[:, at] = total
    seen = jnp.concatenate(read + [jnp.zeros((z.lead - z.heads, n), F32)], axis=0)
    given = by_head(z, two(packed[:, : z.width].astype(F32) * dx[...]))
    later = below(n, n, lambda i, j: i >= j)
    base[...] = given / steps - rates[:, :1] * dots(three(seen - given), later)
    dx[...] = dx[...] + gains[:1, :] * dy[...].astype(F32)
    high, low = two(mixed[...])
    gb[0] = dot(high, c) + dot(low, c)
    gb[1] = dot(high, b, ((0,), (0,))) + dot(low, b, ((0,), (0,)))
    for k in range(modes):
        rows, _ = weighted(z, onward(modes, k), scales[k], packed, dy)
        high, low = two(rows)
        scaled[2 * k] = high
        scaled[2 * k + 1] = low


def arrived(z, state, k):
    parts = []
    for block in range(z.blocks):
        power = state[k, z.blocks * z.state + block : z.blocks * z.state + block + 1, :]
        parts.append(state[k, block * z.state : (block + 1) * z.state, :] * jnp.exp2(power))
    return jnp.concatenate(parts, axis=1)


def chosen(z, forward, packed):
    return jnp.where(
        forward,
        packed[:, z.width : z.width + z.state],
        packed[:, z.width + z.state :],
    )


def carry(basis, high, low):
    return dot(jnp.concatenate([basis, basis], axis=1), jnp.concatenate([high, low], axis=0))


def last_kernel(z, modes, packed, scales, scaled, dx, gb, state, out, own, partner, stage, sem):
    extra = [gb[0], gb[1]]
    states = []
    for k in range(modes):
        forward = onward(modes, k)
        high, low = two(arrived(z, state, k))
        states.append((high, low))
        both = dot(scaled[2 * k], jnp.concatenate([high, low], axis=0), ((1,), (1,)))
        grown = both[:, : z.state] + both[:, z.state :] + dot(scaled[2 * k + 1], high, ((1,), (1,)))
        none = jnp.zeros_like(grown)
        extra = [extra[0] + jnp.where(forward, grown, none), extra[1] + jnp.where(forward, none, grown)]
    chunk = z.tokens // out.shape[0]
    for k in range(out.shape[0]):
        for which in range(2):
            stage[k, which] = extra[which][k * chunk : (k + 1) * chunk, :]
    shares = pltpu.make_async_copy(stage, out, sem)
    shares.start()
    total = dx[...]
    for k in range(modes):
        forward = onward(modes, k)
        carried = carry(chosen(z, forward, packed), *states[k])
        total = total + jnp.where(forward, scales[k], jnp.zeros_like(carried)) * carried
    first = lax.axis_index("member") == 0
    half = z.rows
    early, late = total[:half, :].astype(BF16), total[half:, :].astype(BF16)
    own[...] = jnp.where(first, early, late)
    partner[...] = jnp.where(first, late, early)
    shares.wait()


def step_kernel(z, modes, packed, table, scaled, base, rates, state, own, partner):
    n = z.tokens
    steps = table[: z.lead, :]
    decays = jnp.zeros_like(steps)
    steps_grad = base[...]
    states = []
    for k in range(modes):
        forward = onward(modes, k)
        came = arrived(z, state, k)
        states.append(came)
        carried = carry(chosen(z, forward, packed), *two(came))
        rows = scaled[2 * k].astype(F32) + scaled[2 * k + 1].astype(F32)
        found = by_head(z, two(rows * carried))
        i = lax.broadcasted_iota(jnp.int32, (n, n), 0)
        j = lax.broadcasted_iota(jnp.int32, (n, n), 1)
        reach = (j - i) * jnp.where(forward, 1, -1) >= jnp.where(forward, 1, 0)
        decays = decays + dots(three(found), jnp.where(reach, 1.0, 0.0).astype(BF16))
        steps_grad = steps_grad + jnp.where(forward, found, jnp.zeros_like(found)) / steps
    if modes == 2:
        sums = table[z.lead : 2 * z.lead, :]
        both = by_head(z, three(states[0] * states[1]))
        decays = decays + jnp.sum(both, axis=1, keepdims=True) * jnp.exp(sums[:, -1:])
    steps_grad = steps_grad - rates[:, :1] * decays
    first = lax.axis_index("member") == 0
    early, late = steps_grad[:, : z.rows], steps_grad[:, z.rows :]
    own[...] = jnp.where(first, early, late)
    partner[...] = jnp.where(first, late, early)


def call(kernel, out_shape, arrays, flops, scratch=(), away=0):
    vmem = pl.BlockSpec(memory_space=pltpu.VMEM)
    hbm = pl.BlockSpec(memory_space=pltpu.HBM)
    return pl.pallas_call(
        kernel,
        out_shape=out_shape,
        in_specs=[vmem] * len(arrays),
        out_specs=[hbm] * away + [vmem] * (len(out_shape) - away),
        scratch_shapes=scratch,
        compiler_params=pltpu.CompilerParams(vmem_limit_bytes=40 * 1024 * 1024),
        cost_estimate=pl.CostEstimate(flops=flops, bytes_accessed=2_000_000, transcendentals=0),
    )(*arrays)


def messages(z, peers, grad_out, step_sizes, x_ckpt, bc_ckpt):
    tokens = x_ckpt.shape[0]
    away = pl.BlockSpec(memory_space=pltpu.HBM)
    packed = (peers, tokens, z.width + 2 * z.state)
    return pl.pallas_call(
        partial(open_kernel, z),
        out_shape=[
            jax.ShapeDtypeStruct((z.rows + z.lead, z.width), BF16),
            jax.ShapeDtypeStruct(packed, BF16),
        ],
        in_specs=[away] * 4,
        out_specs=[away, away],
        scratch_shapes=[
            pltpu.VMEM(step_sizes.shape, F32),
            pltpu.VMEM(bc_ckpt.shape, BF16),
            pltpu.VMEM(packed, BF16),
            pltpu.VMEM((z.rows + z.lead, z.width), BF16),
            pltpu.SemaphoreType.DMA((6,)),
        ],
        compiler_params=pltpu.CompilerParams(vmem_limit_bytes=OPENING_VMEM),
    )(grad_out, step_sizes, x_ckpt, bc_ckpt)


def chain(state, passing, size, index, reverse):
    ring = [(i, i + 1) for i in range(size - 1)]
    if reverse:
        ring = [(j, i) for i, j in ring]
    place = size - 1 - index if reverse else index

    def hop(k, carry):
        entering, leaving = carry
        came = lax.ppermute(leaving, "pair", ring)
        here = place == k
        return (
            jnp.where(here, came, entering),
            jnp.where(here, passing * came + state, leaving),
        )

    return lax.fori_loop(1, size, hop, (jnp.zeros_like(state), state))[0]


def shards(x_ckpt, bc_ckpt, step_sizes, decay_rate, skip_gain, grad_out):
    heads, rows = step_sizes.shape
    z = Sizes(heads, rows, grad_out.shape[1], bc_ckpt.shape[2])
    pairs, tp = lax.axis_size("pair"), lax.axis_size("tp")
    pair, member = lax.axis_index("pair"), lax.axis_index("member")
    swap = [(0, 1), (1, 0)]
    modes = 1 if pairs == 2 else 2

    shape = jax.ShapeDtypeStruct
    tokens = x_ckpt.shape[0]
    message, slots = messages(z, 2 * tp, grad_out, step_sizes, x_ckpt, bc_ckpt)
    message = lax.ppermute(message, "member", swap)
    packed = lax.all_to_all(slots, ("member", "tp"), split_axis=0, concat_axis=0, tiled=True)
    packed = packed.reshape(z.tokens, z.width + 2 * z.state)

    mine = lax.dynamic_slice(decay_rate, (member * z.heads,), (z.heads,))
    rates = jnp.broadcast_to(jnp.pad(mine, (0, z.lead - z.heads))[:, None], (z.lead, LANES))
    mine = lax.dynamic_slice(skip_gain, (member * z.heads,), (z.heads,))
    gains = jnp.broadcast_to(jnp.repeat(mine, z.head_width)[None, :], (8, z.width))

    dy, table, scales = call(
        partial(prepare_kernel, z, modes),
        [
            shape((z.tokens, z.width), BF16),
            shape((2 * z.lead, z.tokens), F32),
            shape((modes, z.tokens, z.width), F32),
        ],
        [step_sizes, message, rates, grad_out],
        1_000_000,
    )
    (state,) = call(
        partial(state_kernel, z, modes),
        [shape((modes, z.state_rows, LANES), F32)],
        [packed, dy, table, scales],
        4 * z.tokens * z.state * z.width,
    )
    if modes == 1:
        turn = lax.ppermute(state.astype(jnp.float16), "pair", swap)
        came = turn.astype(F32)
    else:
        body = z.blocks * z.state
        passing = jnp.repeat(state[0, body : body + z.blocks], z.state, axis=0)
        forth = chain(state[0, :body], passing, pairs, pair, False)
        back = chain(state[1, :body], passing, pairs, pair, True)
        came = jnp.pad(jnp.stack([back, forth]), ((0, 0), (0, z.state_rows - body), (0, 0)))

    dx, gb, base, scaled = call(
        partial(local_kernel, z, modes),
        [
            shape((z.tokens, z.width), F32),
            shape((2, z.tokens, z.state), F32),
            shape((z.lead, z.tokens), F32),
            shape((2 * modes, z.tokens, z.width), BF16),
        ],
        [packed, dy, table, scales, rates, gains],
        12 * z.tokens * z.tokens * z.width,
        [pltpu.VMEM((z.tokens, z.tokens), F32)],
    )
    out, own, partner = call(
        partial(last_kernel, z, modes),
        [
            shape((2 * tp, 2, tokens, z.state), F32),
            shape((rows, z.width), BF16),
            shape((rows, z.width), BF16),
        ],
        [packed, scales, scaled, dx, gb, came],
        12 * z.tokens * z.state * z.width,
        [pltpu.VMEM((2 * tp, 2, tokens, z.state), F32), pltpu.SemaphoreType.DMA],
        1,
    )
    theirs = lax.ppermute(partner, "member", swap)
    gathered = lax.all_to_all(out, ("member", "tp"), split_axis=0, concat_axis=0, tiled=True)
    mine, partner = call(
        partial(step_kernel, z, modes),
        [shape((z.lead, rows), F32), shape((z.lead, rows), F32)],
        [packed, table, scaled, base, rates, came],
        4 * z.tokens * z.state * z.width,
    )
    other = lax.ppermute(partner, "member", swap)
    grad_bc = jnp.sum(gathered, axis=0)
    first = member == 0
    grad_x = jnp.where(
        first,
        jnp.concatenate([own, theirs], axis=1),
        jnp.concatenate([theirs, own], axis=1),
    )
    mine, other = mine[: z.heads], other[: z.heads]
    grad_step = jnp.where(
        first,
        jnp.concatenate([mine, other], axis=0),
        jnp.concatenate([other, mine], axis=0),
    )
    return (grad_x, grad_bc, grad_step)


def solution(mesh):
    sizes = dict(mesh.shape)
    names = []
    for name in mesh.axis_names:
        names += ["pair", "member"] if name == "seq" else [name]
    shape = []
    for name in mesh.axis_names:
        shape += [sizes[name] // 2, 2] if name == "seq" else [sizes[name]]
    fine = Mesh(mesh.devices.reshape(shape), tuple(names))
    seq = ("dp", "pair", "member")
    return jax.shard_map(
        shards,
        mesh=fine,
        in_specs=(
            P((*seq, "tp"), None),
            P(None, (*seq, "tp"), None),
            P("tp", seq),
            P("tp"),
            P("tp"),
            P(seq, "tp"),
        ),
        out_specs=(
            P(seq, "tp"),
            P(None, (*seq, "tp"), None),
            P("tp", seq),
        ),
        check_vma=False,
    )
```

```python
from functools import partial

import jax
import jax.numpy as jnp
from jax import lax
from jax.experimental import pallas as pl
from jax.experimental.pallas import tpu as pltpu
from jax.sharding import Mesh, PartitionSpec as P

F32 = jnp.float32
BF16 = jnp.bfloat16
LANES = 128
NEVER = -1e30


def dot(a, b, dims=((1,), (0,))):
    return lax.dot_general(a, b, (dims, ((), ())), preferred_element_type=F32)


def two(a):
    high = a.astype(BF16)
    return high, (a - high.astype(F32)).astype(BF16)


def three(a):
    high = a.astype(BF16)
    rest = a - high.astype(F32)
    mid = rest.astype(BF16)
    return high, mid, (rest - mid.astype(F32)).astype(BF16)


def dots(parts, b, dims=((1,), (0,))):
    total = dot(parts[0], b, dims)
    for part in parts[1:]:
        total = total + dot(part, b, dims)
    return total


def below(rows, cols, test):
    i = lax.broadcasted_iota(jnp.int32, (rows, cols), 0)
    j = lax.broadcasted_iota(jnp.int32, (rows, cols), 1)
    return jnp.where(test(i, j), 1.0, 0.0).astype(BF16)


def lead(heads):
    return -(-heads // 16) * 16


class Sizes:
    def __init__(self, heads, rows, columns, state):
        self.heads = heads // 2
        self.rows = rows
        self.tokens = 2 * rows
        self.width = columns // 2
        self.head_width = self.width // self.heads
        self.state = state
        self.lead = lead(self.heads)
        self.blocks = self.width // LANES
        self.state_rows = self.blocks * state + -(-self.blocks // 8) * 8

    def spread(self):
        return below(self.lead, self.width, lambda i, j: j // self.head_width == i)


def onward(modes, k):
    return lax.axis_index("pair") == 0 if modes == 1 else k == 0


def exponent(a):
    top = jnp.max(jnp.abs(a), axis=0, keepdims=True)
    return jnp.ceil(jnp.log2(jnp.maximum(top, 1e-30)))


def by_head(z, parts):
    spread = z.spread()
    total = dot(spread, parts[0], ((1,), (1,)))
    for part in parts[1:]:
        total = total + dot(spread, part, ((1,), (1,)))
    return total


def tables(z, step, message, rates):
    first = lax.axis_index("member") == 0
    own = jnp.where(first, step[: z.heads, :], step[z.heads :, :])
    if z.lead > z.heads:
        own = jnp.concatenate([own, jnp.ones((z.lead - z.heads, z.rows), F32)], axis=0)
    tail = message[z.rows : z.rows + z.lead, : 3 * z.rows].astype(F32)
    other = tail[:, : z.rows] + tail[:, z.rows : 2 * z.rows] + tail[:, 2 * z.rows : 3 * z.rows]
    steps = jnp.concatenate([jnp.where(first, own, other), jnp.where(first, other, own)], axis=1)
    logs = steps * (-rates[:, :1])
    upto = below(z.tokens, z.tokens, lambda i, j: i <= j)
    return steps, dots(three(logs), upto)


def gradient(z, grad, message):
    first = lax.axis_index("member") == 0
    own = jnp.where(first, grad[:, : z.width], grad[:, z.width :])
    other = message[: z.rows, :]
    return jnp.concatenate([jnp.where(first, own, other), jnp.where(first, other, own)], axis=0)


def send_kernel(z, grad, step, message, held, sems):
    index = lax.axis_index("member")
    first = index == 0
    at = pl.multiple_of((1 - index) * z.width, LANES)
    rows = pltpu.make_async_copy(grad.at[:, pl.ds(at, z.width)], message.at[pl.ds(0, z.rows), :], sems.at[0])
    sizes = pltpu.make_async_copy(step, held, sems.at[1])
    rows.start()
    sizes.start()
    message[z.rows :, :] = jnp.zeros((z.lead, z.width), BF16)
    sizes.wait()
    steps = jnp.where(first, held[z.heads :, :], held[: z.heads, :])
    if z.lead > z.heads:
        steps = jnp.concatenate([steps, jnp.ones((z.lead - z.heads, z.rows), F32)], axis=0)
    for k, part in enumerate(three(steps)):
        message[z.rows :, k * z.rows : (k + 1) * z.rows] = part
    rows.wait()


def pack_kernel(z, x, bc, slots, sem):
    count = slots.shape[0]
    for k in range(count):
        member, peer = divmod(k, count // 2)
        columns = pl.ds((2 * peer + member) * z.width, z.width)
        pltpu.make_async_copy(x.at[:, columns], slots.at[k, :, pl.ds(0, z.width)], sem).start()
        for which in range(2):
            at = pl.ds(z.width + which * z.state, z.state)
            pltpu.make_async_copy(bc.at[which], slots.at[k, :, at], sem).start()
    pltpu.make_async_copy(slots, slots, sem).wait()


def prepare_kernel(z, modes, step, message, rates, grad, dy, table, scales):
    steps, sums = tables(z, step, message, rates)
    dy[...] = gradient(z, grad, message)
    table[: z.lead, :] = steps
    table[z.lead : 2 * z.lead, :] = sums
    tail = steps * jnp.exp(sums[:, -1:] - sums)
    for k in range(modes):
        chosen = jnp.where(onward(modes, k), tail, jnp.exp(sums))
        scales[k] = dots(three(chosen), z.spread(), ((0,), (0,)))


def weighted(z, forward, scale, packed, dy):
    source = jnp.where(forward, packed[:, : z.width], dy[...]).astype(F32)
    basis = jnp.where(
        forward,
        packed[:, z.width : z.width + z.state],
        packed[:, z.width + z.state :],
    )
    return scale * source, basis


def state_kernel(z, modes, packed, dy, table, scales, state):
    for k in range(modes):
        rows, basis = weighted(z, onward(modes, k), scales[k], packed, dy)
        high, low = two(rows)
        found = dot(basis, high, ((0,), (0,))) + dot(basis, low, ((0,), (0,)))
        if modes == 1:
            power = exponent(found)
            found = found * jnp.exp2(-power)
        else:
            sums = table[z.lead : 2 * z.lead, :]
            passing = jnp.broadcast_to(jnp.exp(sums[:, -1:]), (z.lead, LANES))
            power = dots(three(passing), z.spread(), ((0,), (0,)))[:1, :]
        for block in range(z.blocks):
            at = slice(block * LANES, (block + 1) * LANES)
            state[k, block * z.state : (block + 1) * z.state, :] = found[:, at]
            state[k, z.blocks * z.state + block : z.blocks * z.state + block + 1, :] = power[:, at]
        left = state.shape[1] - z.blocks * (z.state + 1)
        if left:
            state[k, z.blocks * (z.state + 1) :, :] = jnp.zeros((left, LANES), F32)


def local_kernel(z, modes, packed, dy, table, scales, rates, gains, dx, gb, base, scaled, mixed):
    n, half = z.tokens, z.rows
    steps = table[: z.lead, :]
    sums = table[z.lead : 2 * z.lead, :]
    source = jnp.log(steps) - sums
    pad = jnp.zeros((LANES - z.lead, n), F32)
    columns = jnp.transpose(jnp.concatenate([source, pad], axis=0))
    b = packed[:, z.width : z.width + z.state]
    c = packed[:, z.width + z.state :]
    scores = dot(b, c, ((1,), (1,)))
    mixed[...] = jnp.zeros((n, n), F32)
    per = LANES // z.head_width
    lane = lax.broadcasted_iota(jnp.int32, (n, LANES), 1) // z.head_width
    read = []
    for block in range(z.width // LANES):
        at = slice(block * LANES, (block + 1) * LANES)
        values = packed[:, at]
        upstream = dy[:, at]
        total = jnp.zeros((n, LANES), F32)
        for k in range(per):
            h = block * per + k
            own = jnp.where(lane == k, upstream, jnp.zeros_like(upstream))
            row = sums[h : h + 1, :]
            pieces = []
            drawn = jnp.zeros((1, n), F32)
            for part in range(2):
                s = slice(part * half, (part + 1) * half)
                t = slice(part * half, n)
                wide = n - part * half
                i = lax.broadcasted_iota(jnp.int32, (half, wide), 0)
                j = lax.broadcasted_iota(jnp.int32, (half, wide), 1)
                gap = row[:, t] + columns[s, h : h + 1]
                decay = jnp.exp(jnp.where(j >= i, gap, NEVER))
                pairs = decay * dot(values[s, :], own[t, :], ((1,), (1,)))
                mixed[s, t] += pairs
                score = scores[s, t]
                seen = jnp.sum(pairs * score, axis=0, keepdims=True)
                if part:
                    seen = jnp.concatenate([jnp.zeros((1, half), F32), seen], axis=1)
                drawn = drawn + seen
                high, low = two(decay * score)
                pieces.append(dot(high, own[t, :]) + dot(low, own[t, :]))
            read.append(drawn)
            total = total + jnp.concatenate(pieces, axis=0)
        dx[:, at] = total
    seen = jnp.concatenate(read + [jnp.zeros((z.lead - z.heads, n), F32)], axis=0)
    given = by_head(z, two(packed[:, : z.width].astype(F32) * dx[...]))
    later = below(n, n, lambda i, j: i >= j)
    base[...] = given / steps - rates[:, :1] * dots(three(seen - given), later)
    dx[...] = dx[...] + gains[:1, :] * dy[...].astype(F32)
    high, low = two(mixed[...])
    gb[0] = dot(high, c) + dot(low, c)
    gb[1] = dot(high, b, ((0,), (0,))) + dot(low, b, ((0,), (0,)))
    for k in range(modes):
        rows, _ = weighted(z, onward(modes, k), scales[k], packed, dy)
        high, low = two(rows)
        scaled[2 * k] = high
        scaled[2 * k + 1] = low


def arrived(z, state, k):
    parts = []
    for block in range(z.blocks):
        power = state[k, z.blocks * z.state + block : z.blocks * z.state + block + 1, :]
        parts.append(state[k, block * z.state : (block + 1) * z.state, :] * jnp.exp2(power))
    return jnp.concatenate(parts, axis=1)


def chosen(z, forward, packed):
    return jnp.where(
        forward,
        packed[:, z.width : z.width + z.state],
        packed[:, z.width + z.state :],
    )


def carry(basis, high, low):
    return dot(jnp.concatenate([basis, basis], axis=1), jnp.concatenate([high, low], axis=0))


def last_kernel(z, modes, packed, scales, scaled, dx, gb, state, out, own, partner, stage, sem):
    extra = [gb[0], gb[1]]
    states = []
    for k in range(modes):
        forward = onward(modes, k)
        high, low = two(arrived(z, state, k))
        states.append((high, low))
        both = dot(scaled[2 * k], jnp.concatenate([high, low], axis=0), ((1,), (1,)))
        grown = both[:, : z.state] + both[:, z.state :] + dot(scaled[2 * k + 1], high, ((1,), (1,)))
        none = jnp.zeros_like(grown)
        extra = [extra[0] + jnp.where(forward, grown, none), extra[1] + jnp.where(forward, none, grown)]
    chunk = z.tokens // out.shape[0]
    for k in range(out.shape[0]):
        for which in range(2):
            stage[k, which] = extra[which][k * chunk : (k + 1) * chunk, :]
    shares = pltpu.make_async_copy(stage, out, sem)
    shares.start()
    total = dx[...]
    for k in range(modes):
        forward = onward(modes, k)
        carried = carry(chosen(z, forward, packed), *states[k])
        total = total + jnp.where(forward, scales[k], jnp.zeros_like(carried)) * carried
    first = lax.axis_index("member") == 0
    half = z.rows
    early, late = total[:half, :].astype(BF16), total[half:, :].astype(BF16)
    own[...] = jnp.where(first, early, late)
    partner[...] = jnp.where(first, late, early)
    shares.wait()


def step_kernel(z, modes, packed, table, scaled, base, rates, state, own, partner):
    n = z.tokens
    steps = table[: z.lead, :]
    decays = jnp.zeros_like(steps)
    steps_grad = base[...]
    states = []
    for k in range(modes):
        forward = onward(modes, k)
        came = arrived(z, state, k)
        states.append(came)
        carried = carry(chosen(z, forward, packed), *two(came))
        rows = scaled[2 * k].astype(F32) + scaled[2 * k + 1].astype(F32)
        found = by_head(z, two(rows * carried))
        i = lax.broadcasted_iota(jnp.int32, (n, n), 0)
        j = lax.broadcasted_iota(jnp.int32, (n, n), 1)
        reach = (j - i) * jnp.where(forward, 1, -1) >= jnp.where(forward, 1, 0)
        decays = decays + dots(three(found), jnp.where(reach, 1.0, 0.0).astype(BF16))
        steps_grad = steps_grad + jnp.where(forward, found, jnp.zeros_like(found)) / steps
    if modes == 2:
        sums = table[z.lead : 2 * z.lead, :]
        both = by_head(z, three(states[0] * states[1]))
        decays = decays + jnp.sum(both, axis=1, keepdims=True) * jnp.exp(sums[:, -1:])
    steps_grad = steps_grad - rates[:, :1] * decays
    first = lax.axis_index("member") == 0
    early, late = steps_grad[:, : z.rows], steps_grad[:, z.rows :]
    own[...] = jnp.where(first, early, late)
    partner[...] = jnp.where(first, late, early)


def call(kernel, out_shape, arrays, flops, scratch=(), away=0, space=pltpu.VMEM):
    vmem = pl.BlockSpec(memory_space=pltpu.VMEM)
    hbm = pl.BlockSpec(memory_space=pltpu.HBM)
    return pl.pallas_call(
        kernel,
        out_shape=out_shape,
        in_specs=[pl.BlockSpec(memory_space=space)] * len(arrays),
        out_specs=[hbm] * away + [vmem] * (len(out_shape) - away),
        scratch_shapes=scratch,
        compiler_params=pltpu.CompilerParams(vmem_limit_bytes=40 * 1024 * 1024),
        cost_estimate=pl.CostEstimate(flops=flops, bytes_accessed=2_000_000, transcendentals=0),
    )(*arrays)


def chain(state, passing, size, index, reverse):
    ring = [(i, i + 1) for i in range(size - 1)]
    if reverse:
        ring = [(j, i) for i, j in ring]
    place = size - 1 - index if reverse else index

    def hop(k, carry):
        entering, leaving = carry
        came = lax.ppermute(leaving, "pair", ring)
        here = place == k
        return (
            jnp.where(here, came, entering),
            jnp.where(here, passing * came + state, leaving),
        )

    return lax.fori_loop(1, size, hop, (jnp.zeros_like(state), state))[0]


def shards(x_ckpt, bc_ckpt, step_sizes, decay_rate, skip_gain, grad_out):
    heads, rows = step_sizes.shape
    z = Sizes(heads, rows, grad_out.shape[1], bc_ckpt.shape[2])
    pairs, tp = lax.axis_size("pair"), lax.axis_size("tp")
    pair, member = lax.axis_index("pair"), lax.axis_index("member")
    swap = [(0, 1), (1, 0)]
    modes = 1 if pairs == 2 else 2

    shape = jax.ShapeDtypeStruct
    tokens = x_ckpt.shape[0]
    (message,) = call(
        partial(send_kernel, z),
        [shape((rows + z.lead, z.width), BF16)],
        [pltpu.with_memory_space_constraint(a, pltpu.HBM) for a in (grad_out, step_sizes)],
        1000,
        [pltpu.VMEM((heads, rows), F32), pltpu.SemaphoreType.DMA((2,))],
        space=pltpu.HBM,
    )
    message = lax.ppermute(message, "member", swap)
    (slots,) = call(
        partial(pack_kernel, z),
        [shape((2 * tp, tokens, z.width + 2 * z.state), BF16)],
        [x_ckpt, bc_ckpt],
        1000,
        [pltpu.SemaphoreType.DMA],
        1,
    )
    packed = lax.all_to_all(slots, ("member", "tp"), split_axis=0, concat_axis=0, tiled=True)
    packed = packed.reshape(z.tokens, z.width + 2 * z.state)

    mine = lax.dynamic_slice(decay_rate, (member * z.heads,), (z.heads,))
    rates = jnp.broadcast_to(jnp.pad(mine, (0, z.lead - z.heads))[:, None], (z.lead, LANES))
    mine = lax.dynamic_slice(skip_gain, (member * z.heads,), (z.heads,))
    gains = jnp.broadcast_to(jnp.repeat(mine, z.head_width)[None, :], (8, z.width))

    dy, table, scales = call(
        partial(prepare_kernel, z, modes),
        [
            shape((z.tokens, z.width), BF16),
            shape((2 * z.lead, z.tokens), F32),
            shape((modes, z.tokens, z.width), F32),
        ],
        [step_sizes, message, rates, grad_out],
        1_000_000,
    )
    (state,) = call(
        partial(state_kernel, z, modes),
        [shape((modes, z.state_rows, LANES), F32)],
        [packed, dy, table, scales],
        4 * z.tokens * z.state * z.width,
    )
    if modes == 1:
        turn = lax.ppermute(state.astype(jnp.float16), "pair", swap)
        came = turn.astype(F32)
    else:
        body = z.blocks * z.state
        passing = jnp.repeat(state[0, body : body + z.blocks], z.state, axis=0)
        forth = chain(state[0, :body], passing, pairs, pair, False)
        back = chain(state[1, :body], passing, pairs, pair, True)
        came = jnp.pad(jnp.stack([back, forth]), ((0, 0), (0, z.state_rows - body), (0, 0)))

    dx, gb, base, scaled = call(
        partial(local_kernel, z, modes),
        [
            shape((z.tokens, z.width), F32),
            shape((2, z.tokens, z.state), F32),
            shape((z.lead, z.tokens), F32),
            shape((2 * modes, z.tokens, z.width), BF16),
        ],
        [packed, dy, table, scales, rates, gains],
        12 * z.tokens * z.tokens * z.width,
        [pltpu.VMEM((z.tokens, z.tokens), F32)],
    )
    out, own, partner = call(
        partial(last_kernel, z, modes),
        [
            shape((2 * tp, 2, tokens, z.state), F32),
            shape((rows, z.width), BF16),
            shape((rows, z.width), BF16),
        ],
        [packed, scales, scaled, dx, gb, came],
        12 * z.tokens * z.state * z.width,
        [pltpu.VMEM((2 * tp, 2, tokens, z.state), F32), pltpu.SemaphoreType.DMA],
        1,
    )
    theirs = lax.ppermute(partner, "member", swap)
    gathered = lax.all_to_all(out, ("member", "tp"), split_axis=0, concat_axis=0, tiled=True)
    mine, partner = call(
        partial(step_kernel, z, modes),
        [shape((z.lead, rows), F32), shape((z.lead, rows), F32)],
        [packed, table, scaled, base, rates, came],
        4 * z.tokens * z.state * z.width,
    )
    other = lax.ppermute(partner, "member", swap)
    grad_bc = jnp.sum(gathered, axis=0)
    first = member == 0
    grad_x = jnp.where(
        first,
        jnp.concatenate([own, theirs], axis=1),
        jnp.concatenate([theirs, own], axis=1),
    )
    mine, other = mine[: z.heads], other[: z.heads]
    grad_step = jnp.where(
        first,
        jnp.concatenate([mine, other], axis=0),
        jnp.concatenate([other, mine], axis=0),
    )
    return (grad_x, grad_bc, grad_step)


def solution(mesh):
    sizes = dict(mesh.shape)
    names = []
    for name in mesh.axis_names:
        names += ["pair", "member"] if name == "seq" else [name]
    shape = []
    for name in mesh.axis_names:
        shape += [sizes[name] // 2, 2] if name == "seq" else [sizes[name]]
    fine = Mesh(mesh.devices.reshape(shape), tuple(names))
    seq = ("dp", "pair", "member")
    return jax.shard_map(
        shards,
        mesh=fine,
        in_specs=(
            P((*seq, "tp"), None),
            P(None, (*seq, "tp"), None),
            P("tp", seq),
            P("tp"),
            P("tp"),
            P(seq, "tp"),
        ),
        out_specs=(
            P(seq, "tp"),
            P(None, (*seq, "tp"), None),
            P("tp", seq),
        ),
        check_vma=False,
    )
```
